256 devices in a mesh: gx: 32 (over x, z), gy: 4 (over y), gz: 2 (over core).
Axes of the slice: x: 4, y: 4, z: 8, core: 2. Of those that a mesh axis runs over, the one named last changes fastest.
Arguments:
- coarse_field: float32 [3, 1024, 128, 512], P(None, 'gx', 'gy', 'gz'), may hold values from -6 to 6
- fine_field: float32 [3, 1024, 16, 256], P(None, ('gx', 'gy', 'gz')), may hold values from -6 to 6
- viscosity: float32 [1024, 16, 256], P(('gx', 'gy', 'gz')), may hold values from 0.1 to 1
- corners: int32 [512, 3], replicated, may hold values from 0 to 1016, as said below
- grid_slot: int32 [512], replicated, may hold values from 0 to 1023, as said below
- neighbors: int32 [512, 2], replicated, may hold values from -1 to 511, as said below
Outputs:
- fine_out: float32 [3, 1024, 16, 256], P(None, ('gx', 'gy', 'gz'))
- coarse_out: float32 [3, 1024, 128, 512], P(None, 'gx', 'gy', 'gz')
The draws below stay inside these ranges and needn't reach their ends.
Inputs may be any that keep to these rules, and one draw needn't show every extreme that they name: Each box is 8 coarse cells on a side, its corner coordinates are multiples of 8, it lies inside the domain and inside one coarse brick of 32 x 32 x 256 cells, and different grids have different boxes. A brick holds either no box or exactly 4 boxes, which share their y and z corners and are grids of one wake. `grid_slot`: different grids have different slots. A grid's slot lies on a device with the same gz index as the brick that holds its box. Every device holds at most 4 grids, some device holds 4 grids in every draw, and all grids of one device lie in one brick. `neighbors`: entry 0 is the grid of the same wake whose box touches the grid's lower x face, entry 1 the one touching its upper x face, or -1 where there is none.
All inputs are finite; a program needn't handle non-finite values.
Results may differ from the reference program's by a relative error of at most 0.00005.
Values sent between devices are 32-bit elements; how exact they have to be, the bound alone decides.
A program may use at most 128 MiB of HBM per device.

```python
import math
import jax
import jax.numpy as jnp
from jax import lax

B = 8
F = 16
CY = 32
CZ = 256
SLOTS = 4
WAKE = 8
NX = 1024
NY = 128
NZ = 512
N_GX = 32
N_GY = 4
N_GZ = 2


def wind_layout(key):
    root_random_key = jax.random.fold_in(key, 4242)
    groups = N_GX * N_GY
    turbines = groups // 4
    half_x = N_GX // 2
    pair_count = groups // 2
    rows_z = CZ // B
    grid_count = turbines * WAKE
    corner_parts = []
    slot_parts = []
    near_parts = []
    for z_layer in range(N_GZ):
        subkeys = jax.random.split(jax.random.fold_in(root_random_key, z_layer), 7)
        pair_order = jax.random.permutation(subkeys[0], pair_count).astype(jnp.int32)
        first_pair = jax.random.randint(subkeys[1], (), half_x, pair_count, dtype=jnp.int32)
        found_at = jnp.argmax(pair_order == first_pair).astype(jnp.int32)
        pair_order = pair_order.at[found_at].set(pair_order[0]).at[0].set(first_pair)
        chosen = pair_order[:turbines]
        brick_row = chosen // half_x
        brick_first = 2 * (chosen % half_x)
        edge_z = rows_z - 1 if z_layer % 2 == 0 else 0
        inner_y = jax.random.randint(subkeys[2], (turbines,), 0, CY // B, dtype=jnp.int32).at[0].set(0)
        inner_z = jax.random.randint(subkeys[5], (turbines,), 0, rows_z, dtype=jnp.int32).at[0].set(edge_z)
        row_y = brick_row * (CY // B) + inner_y
        row_z = inner_z + z_layer * rows_z
        start_x = brick_first * SLOTS
        along_wake = jnp.arange(WAKE, dtype=jnp.int32)
        lattice_x = (start_x[:, None] + along_wake[None, :]).reshape(-1)
        lattice_y = jnp.repeat(row_y, WAKE)
        lattice_z = jnp.repeat(row_z, WAKE)
        corner_parts.append((jnp.stack([lattice_x, lattice_y, lattice_z], axis=1) * B).astype(jnp.int32))
        local_ids = jnp.arange(grid_count, dtype=jnp.int32)
        global_ids = local_ids + z_layer * grid_count
        in_wake = local_ids % WAKE
        near_parts.append(jnp.stack([jnp.where(in_wake > 0, global_ids - 1, -1), jnp.where(in_wake < WAKE - 1, global_ids + 1, -1)], axis=1).astype(jnp.int32))
        devices = jax.random.permutation(subkeys[3], groups).astype(jnp.int32)
        across = (devices[0] + groups // 2) % groups
        across_at = jnp.argmax(devices == across).astype(jnp.int32)
        devices = devices.at[across_at].set(devices[2]).at[2].set(across)
        second_share = jax.random.randint(subkeys[6], (), 1, SLOTS + 1, dtype=jnp.int32)
        shares = jax.random.randint(subkeys[4], (groups // 2,), 0, SLOTS + 1, dtype=jnp.int32).at[0].set(SLOTS).at[1].set(second_share)
        half_id = local_ids // SLOTS
        inside = local_ids % SLOTS
        share_limit = shares[half_id]
        owner_group = jnp.where(inside < share_limit, devices[2 * half_id], devices[2 * half_id + 1])
        owner_slot = jnp.where(inside < share_limit, inside, inside - share_limit)
        slot_parts.append(((owner_group * N_GZ + z_layer) * SLOTS + owner_slot).astype(jnp.int32))
    corner_table = jnp.concatenate(corner_parts, axis=0)
    slot_table = jnp.concatenate(slot_parts, axis=0)
    near_all = jnp.concatenate(near_parts, axis=0)
    total_count = corner_table.shape[0]
    renumbered_slots = jax.random.permutation(jax.random.fold_in(root_random_key, 777), total_count).astype(jnp.int32)
    inverse_permutation = jnp.argsort(renumbered_slots).astype(jnp.int32)
    mapped_neighbor_slots = jnp.where(near_all >= 0, inverse_permutation[jnp.maximum(near_all, 0)], -1).astype(jnp.int32)
    return (corner_table[renumbered_slots], slot_table[renumbered_slots], mapped_neighbor_slots[renumbered_slots])


def draw_corners(key, part):
    return wind_layout(key)[0]


def draw_grid_slot(key, part):
    return wind_layout(key)[1]


def draw_neighbors(key, part):
    return wind_layout(key)[2]


def steps_of(key, dims, pieces, least, high):
    def one(axis_at, shards_of):
        heights = jax.random.uniform(jax.random.fold_in(jax.random.fold_in(key, 6), axis_at), (shards_of,), jnp.float32, least / len(pieces), high / len(pieces))
        return jnp.repeat(jnp.exp(heights), dims[axis_at] // shards_of).reshape((-1,) + (1,) * (len(dims) - axis_at - 1))

    factor_of = one(*pieces[0])
    for cut in pieces[1:]:
        factor_of = factor_of * one(*cut)
    return factor_of


def centred(own_key, shape, scale, reach, pieces=(), held_as=jnp.bfloat16):
    result = scale * jax.random.normal(own_key, shape, jnp.float32)
    if pieces:
        result = result * steps_of(own_key, shape, pieces, -0.22, 0.18)
    return jnp.clip(result, -reach, reach).astype(held_as)


def setup_inputs(seed: int = 0) -> dict:
    keys = jax.random.split(jax.random.key(seed), 7)
    return {
        "coarse_field": centred(keys[0], (3, NX, NY, NZ), 1.0, 6.0, ((1, 32), (2, 4), (3, 2)), jnp.float32),
        "fine_field": centred(keys[1], (3, N_GX * N_GY * N_GZ * SLOTS, F, F * F), 1.0, 6.0, ((1, 256),), jnp.float32),
        "viscosity": jnp.clip(jnp.exp(math.log(1.0) - 2.3025851 * jax.random.uniform(keys[2], (N_GX * N_GY * N_GZ * SLOTS, F, F * F), jnp.float32) ** steps_of(keys[2], (N_GX * N_GY * N_GZ * SLOTS, F, F * F), ((0, 256),), -0.2, 0.2)), 0.1, 1.0),
        "corners": draw_corners(jax.random.fold_in(keys[6], 71), 0),
        "grid_slot": draw_grid_slot(jax.random.fold_in(keys[6], 71), 0),
        "neighbors": draw_neighbors(jax.random.fold_in(keys[6], 71), 0),
    }


step_rate = 0.15


def tables():
    side = B + 2
    fine_index = jnp.arange(F, dtype=jnp.int32)
    coarse_index = jnp.arange(side, dtype=jnp.int32)
    center = fine_index // 2 + 1
    other = jnp.where(fine_index % 2 == 0, center - 1, center + 1)
    tangent = 0.75 * (coarse_index[None, :] == center[:, None]).astype(jnp.float32) + 0.25 * (coarse_index[None, :] == other[:, None]).astype(jnp.float32)
    low_side = 0.75 * (coarse_index == 0).astype(jnp.float32) + 0.25 * (coarse_index == 1).astype(jnp.float32)
    high_side = 0.75 * (coarse_index == side - 1).astype(jnp.float32) + 0.25 * (coarse_index == side - 2).astype(jnp.float32)
    return tangent, low_side, high_side


def advance(volume, visc_cells, ghost_faces, lower_plane, upper_plane):
    components = volume.shape[0]
    slots_here = volume.shape[1]
    cells_edge = volume.shape[2]
    plane_size = volume.shape[3]
    lane_ids = jnp.arange(plane_size, dtype=jnp.int32)
    lane_y = lane_ids // cells_edge
    lane_z = lane_ids % cells_edge
    x_minus = jnp.concatenate([lower_plane[:, :, None], volume[:, :, :-1]], axis=2)
    x_plus = jnp.concatenate([volume[:, :, 1:], upper_plane[:, :, None]], axis=2)
    shape_four = (components, slots_here, cells_edge, cells_edge)
    y_low = jnp.tile(ghost_faces[:, :, 2].reshape(shape_four), (1, 1, 1, cells_edge))
    y_high = jnp.tile(ghost_faces[:, :, 3].reshape(shape_four), (1, 1, 1, cells_edge))
    z_low = jnp.repeat(ghost_faces[:, :, 4].reshape(shape_four), cells_edge, axis=3)
    z_high = jnp.repeat(ghost_faces[:, :, 5].reshape(shape_four), cells_edge, axis=3)
    zero_row = jnp.zeros_like(volume[..., :cells_edge])
    zero_cell = jnp.zeros_like(volume[..., :1])
    y_minus = jnp.where(lane_y == 0, y_low, jnp.concatenate([zero_row, volume[..., :-cells_edge]], axis=-1))
    y_plus = jnp.where(lane_y == cells_edge - 1, y_high, jnp.concatenate([volume[..., cells_edge:], zero_row], axis=-1))
    z_minus = jnp.where(lane_z == 0, z_low, jnp.concatenate([zero_cell, volume[..., :-1]], axis=-1))
    z_plus = jnp.where(lane_z == cells_edge - 1, z_high, jnp.concatenate([volume[..., 1:], zero_cell], axis=-1))
    neighbor_sum = x_minus + x_plus + y_minus + y_plus + z_minus + z_plus - 6.0 * volume
    return volume + step_rate * visc_cells[None] * neighbor_sum


def reference(coarse_field, fine_field, viscosity, corners, grid_slot, neighbors):
    slot_total = fine_field.shape[1]
    grid_total = corners.shape[0]
    grid_ids = jnp.arange(grid_total, dtype=jnp.int32)
    slot_ids = jnp.arange(slot_total, dtype=jnp.int32)
    slot_match = grid_slot[None, :] == slot_ids[:, None]
    slot_active = jnp.any(slot_match, axis=1)
    slot_grid = jnp.sum(jnp.where(slot_match, grid_ids[None, :], 0), axis=1).astype(jnp.int32)
    box_corner = corners[slot_grid].astype(jnp.int32)
    padded = jnp.pad(coarse_field, ((0, 0), (1, 1), (1, 1), (1, 1)))
    zero_start = jnp.zeros((), jnp.int32)

    def cut_cube(corner):
        return lax.dynamic_slice(padded, (zero_start, corner[0], corner[1], corner[2]), (3, B + 2, B + 2, B + 2))

    cubes = jax.vmap(cut_cube)(box_corner)
    tangent, low_side, high_side = tables()
    highest = lax.Precision.HIGHEST
    face_list = [
        jnp.einsum('nkabc,a,sb,tc->knst', cubes, low_side, tangent, tangent, precision=highest),
        jnp.einsum('nkabc,a,sb,tc->knst', cubes, high_side, tangent, tangent, precision=highest),
        jnp.einsum('nkabc,sa,b,tc->knst', cubes, tangent, low_side, tangent, precision=highest),
        jnp.einsum('nkabc,sa,b,tc->knst', cubes, tangent, high_side, tangent, precision=highest),
        jnp.einsum('nkabc,sa,tb,c->knst', cubes, tangent, tangent, low_side, precision=highest),
        jnp.einsum('nkabc,sa,tb,c->knst', cubes, tangent, tangent, high_side, precision=highest),
    ]
    ghost_faces = jnp.stack([face.reshape(3, slot_total, F * F) for face in face_list], axis=2)
    near_grid = neighbors[slot_grid]
    near_slot = grid_slot[jnp.maximum(near_grid, 0)]
    from_low = fine_field[:, near_slot[:, 0], F - 1, :]
    from_high = fine_field[:, near_slot[:, 1], 0, :]
    has_near = (near_grid >= 0) & slot_active[:, None]
    lower_plane = jnp.where(has_near[None, :, 0, None], from_low, ghost_faces[:, :, 0])
    upper_plane = jnp.where(has_near[None, :, 1, None], from_high, ghost_faces[:, :, 1])
    advanced = advance(fine_field, viscosity, ghost_faces, lower_plane, upper_plane)
    fine_out = jnp.where(slot_active[None, :, None, None], advanced, 0.0)
    averages = advanced.reshape(3, slot_total, B, 2, B, 2, B, 2).mean(axis=(3, 5, 7))

    def place_box(index, field_now):
        corner = box_corner[index]
        start = (zero_start, corner[0], corner[1], corner[2])
        current = lax.dynamic_slice(field_now, start, (3, B, B, B))
        value = jnp.where(slot_active[index], averages[:, index], current)
        return lax.dynamic_update_slice(field_now, value, start)

    coarse_out = lax.fori_loop(0, slot_total, place_box, coarse_field)
    return fine_out, coarse_out
```

```python
import numpy as np
import jax
import jax.numpy as jnp
from jax import lax
from jax.experimental import pallas as pl
from jax.experimental.pallas import tpu as pltpu
from jax.sharding import Mesh
from jax.sharding import PartitionSpec as P

MESH = pl.DeviceIdType.MESH
VMEM = pltpu.VMEM
GX = ("gx_0", "gx_1")
GX_GY_GZ = ("gx_0", "gx_1", "gy", "gz")
B = 8
F = 16
SLOTS = 4
NXC, NZC, NYC = 4, 8, 4
HIGH = lax.Precision.HIGHEST
RATE = 0.15
PITCH = 40

T_WIN = 0
T_D = 64
T_P = 72
T_V = 136
T_OD = 168
T_OP = 169
T_OV = 177
T_ACT = 181
T_NEAR = 185
T_Q = 193
T_HERE = 197
T_SIZE = 256


def interpolation():
    t = np.zeros((F, B + 2), np.float32)
    for i in range(F):
        center = i // 2 + 1
        t[i, center] += 0.75
        t[i, center - 1 if i % 2 == 0 else center + 1] += 0.25
    return t


def constants():
    t = interpolation()
    low = np.zeros(B + 2, np.float32)
    low[0], low[1] = 0.75, 0.25
    high = low[::-1]
    side = np.zeros((3, 128, 128), np.float32)
    for c in range(3):
        for a in range(B + 2):
            for b in range(B + 2):
                side[c, a * 10 + b, c * 40 + b] += low[a]
                side[c, a * 10 + b, c * 40 + 10 + b] += high[a]
                side[c, a * 10 + b, c * 40 + 20 + a] += low[b]
                side[c, a * 10 + b, c * 40 + 30 + a] += high[b]
    along = np.zeros((SLOTS * F, 40), np.float32)
    for q in range(SLOTS):
        for i in range(F):
            for a in range(B + 2):
                x = 8 * q - 1 + a
                along[q * F + i, 32 if x < 0 else 33 if x > 31 else x] += t[i, a]
    spread = np.zeros((128, 3, F, F), np.float32)
    for c in range(3):
        for u in range(B + 2):
            spread[c * 40 + u, c, 0, :] += t[:, u]
            spread[c * 40 + 10 + u, c, F - 1, :] += t[:, u]
            spread[c * 40 + 20 + u, c, :, 0] += t[:, u]
            spread[c * 40 + 30 + u, c, :, F - 1] += t[:, u]
    face = np.zeros((128, F, F), np.float32)
    face[:100] = np.einsum("ja,lb->abjl", t, t).reshape(100, F, F)
    pair_yz = np.zeros((2, F, F, 128), np.float32)
    for h in range(2):
        for j in range(F):
            for l in range(F):
                pair_yz[h, j, l, h * 64 + (7 - j // 2) * 8 + l // 2] = 0.25
    pair_x = np.zeros((2, 48, 3, SLOTS, F), np.float32)
    for h in range(2):
        for s in range(SLOTS):
            for c in range(3):
                for r in range(4):
                    row = s * 8 + c * 4 + r if c < 2 else 32 + s * 4 + r
                    pair_x[h, row, c, s, 4 * r + 2 * h : 4 * r + 2 * h + 2] = 0.5
    return (
        side,
        along,
        spread.reshape(128, 3 * F * F),
        face.reshape(128, F * F),
        pair_yz.reshape(2, F * F, 128),
        pair_x.reshape(2, 48, 3 * SLOTS * F),
    )


def index_table(corners, grid_slot, neighbors):
    ix, iz = lax.axis_index("gx_0"), lax.axis_index("gx_1")
    iy, ik = lax.axis_index("gy"), lax.axis_index("gz")
    i32 = jnp.int32
    grids = jnp.arange(corners.shape[0], dtype=i32)
    cx, cy, cz = corners[:, 0], corners[:, 1], corners[:, 2]
    brick = (cx // 32 * NYC + cy // 32) * 2 + cz // 256
    box = cx // B % SLOTS
    place = cy % 32 * 256 + cz % 256
    match = neighbors[:, :, None] == grids[None, None, :]
    near_slot = jnp.sum(jnp.where(match, grid_slot[None, None, :] + 1, 0), axis=2) - 1

    def pick(mask, value):
        return jnp.max(jnp.where(mask, value, -1), axis=-1)

    dy, dk, dx = np.meshgrid([-1, 0, 1], [0, 1], [-1, 0, 1], indexing="ij")
    dy, dk, dx = (jnp.asarray(v.reshape(-1), i32) for v in (dy, dk, dx))
    bx = (ix * NZC + iz + dx) % 32
    by = (iy + dy) % NYC
    bk = (ik + dk) % 2
    near_brick = (bx * NYC + by) * 2 + bk
    found = jnp.maximum(pick(near_brick[:, None] == brick[None, :], place[None, :]), 0)
    win = jnp.stack([found // 256 + (by - iy) * 32, found % 256 + (bk - ik) * 256], axis=1)
    step = jnp.arange(NZC, dtype=i32)
    to_z = (iz + step) % NZC
    device = ((ix * NZC + to_z) * NYC + iy) * 2 + ik
    slot = device[:, None] * SLOTS + jnp.arange(SLOTS, dtype=i32)
    own = slot[:, :, None] == grid_slot
    slot_brick = pick(own, brick)
    slot_box = pick(own, box)
    slot_near = jnp.stack([pick(own, near_slot[:, 0]), pick(own, near_slot[:, 1])], axis=2)
    source = jnp.maximum(jnp.max(slot_brick, axis=1), 0)

    def turn(x, y):
        return (ix - x) % NXC * NYC + (iy - y) % NYC

    def lies(n):
        return n // 64, n // 8 % NZC, n // 2 % NYC

    sx, sz, sy = lies(source)
    t_d = jnp.where(sz == iz, turn(sx, sy), 0)
    near = jnp.maximum(slot_near, 0)
    px, pz, py = lies(near // SLOTS)
    sides = jnp.arange(2, dtype=i32)
    t_p = jnp.where(pz == iz, turn(px, py) * 8 + near % SLOTS * 2 + sides, 0)
    here = (brick == device[:, None])[:, None, :] & (box == jnp.arange(SLOTS, dtype=i32)[:, None])[None]
    home = pick(here, grid_slot)
    held = jnp.maximum(home, 0)
    vx, vz, vy = lies(held // SLOTS)
    t_v = jnp.where(vz == iz, turn(vx, vy) * SLOTS + held % SLOTS, 0)
    parts = [
        win.reshape(-1),
        jnp.zeros(T_D - 36, i32),
        t_d,
        t_p.reshape(-1),
        t_v.reshape(-1),
        (iz - sz[:1]) % NZC,
        ((iz - pz[0]) % NZC).reshape(-1),
        (iz - vz[0]) % NZC,
        (slot_brick[0] >= 0).astype(i32),
        (slot_near[0] >= 0).astype(i32).reshape(-1),
        jnp.maximum(slot_box[0], 0),
        (jnp.max(home[0]) >= 0).astype(i32)[None],
        jnp.zeros(T_SIZE - T_HERE - 1, i32),
    ]
    return jnp.concatenate(parts)


def window_kernel(tab, coarse, own, other, beside, brick, sems):
    copies = [
        pltpu.make_async_copy(
            coarse.at[:, :, :, pl.ds(h * 128, 128)], brick.at[h, :, :, pl.ds(0, 32), :], sems.at[h]
        )
        for h in range(2)
    ]
    for copy in copies:
        copy.start()
    flat = brick.reshape(2 * 3 * 32 * PITCH, 128)
    lane = lax.broadcasted_iota(jnp.int32, (1, 128), 1)
    sub = lax.broadcasted_iota(jnp.int32, (8, 128), 0)

    class Window:
        def __init__(self, dy, core, dx):
            at = T_WIN + 2 * ((dy + 1) * 6 + core * 3 + dx + 1)
            self.y, self.z = tab[at], tab[at + 1]
            z = self.z & 255
            self.half, shift = z >> 7, z & 127
            self.first = (shift - 1) & 127
            self.cross = ((shift == 0) & (lane == 127)) | ((shift == 120) & (lane == 0))

        def row(self, c, yy, base, x=None):
            y = self.y - 1 + yy
            inside = (y >= 0) & (y < 32)
            y = jnp.clip(y, 0, 31)

            def take(half):
                start = half * (3 * 32 * PITCH) + c * (32 * PITCH) + y
                if x is None:
                    return flat[pl.ds(start, 32, stride=PITCH), :]
                return flat[pl.ds(start + x * PITCH, 1), :]

            line = jnp.where(self.cross, take(1 - self.half), take(self.half))
            line = pltpu.roll(line, (base - self.first) & 127, 1)
            t = lane - base
            z = self.z - 1 + t
            keep = (t >= 0) & (t < 10) & (z >= 0) & (z < 256) & inside
            return jnp.where(keep, line, 0.0)

    for copy in copies:
        copy.wait()
    for core, out in ((0, own), (1, other)):
        mid, left, right = (Window(0, core, dx) for dx in (0, -1, 1))
        for c in range(3):
            body = jnp.zeros((32, 128), jnp.float32)
            low = jnp.zeros((1, 128), jnp.float32)
            high = jnp.zeros((1, 128), jnp.float32)
            for yy in range(10):
                body += mid.row(c, yy, yy * 10)
                low += right.row(c, yy, yy * 10, 31)
                high += left.row(c, yy, yy * 10, 0)
            out[c, 0:32, :] = body
            out[c, 32:40, :] = jnp.where(sub == 0, low, jnp.where(sub == 1, high, 0.0))
    for n, (dy, core) in enumerate(((-1, 0), (-1, 1), (1, 0), (1, 1))):
        yy = 9 if dy < 0 else 0
        mid, left, right = (Window(dy, core, dx) for dx in (0, -1, 1))
        body = jnp.zeros((32, 128), jnp.float32)
        low = jnp.zeros((1, 128), jnp.float32)
        high = jnp.zeros((1, 128), jnp.float32)
        for c in range(3):
            body += mid.row(c, yy, c * 10)
            low += right.row(c, yy, c * 10, 31)
            high += left.row(c, yy, c * 10, 0)
        beside[n, 0:32, :] = body
        beside[n, 32:40, :] = jnp.where(sub == 0, low, jnp.where(sub == 1, high, 0.0))


def dot(a, b):
    return jnp.dot(a, b, precision=HIGH, preferred_element_type=jnp.float32)


def exchange_kernel(
    tab, fine, visc, own, other, beside, side, along, spread, face, pair_yz, pair_x,
    fine_out, boxes,
    planes, near_z, near_y, edge, edges, ghost, planes_in, ghost_in, planes_to, ghost_to,
    planes_at, ghost_at, pull, adv, means, means_in, means_to, means_at,
    y_send, y_recv, x_send, x_recv, p_send, p_recv, g_send, g_recv, m_send, m_recv,
    pz_send, pz_recv, gz_send, gz_recv, mz_send, mz_recv,
):
    ix, iz = lax.axis_index("gx_0"), lax.axis_index("gx_1")
    iy, ik = lax.axis_index("gy"), lax.axis_index("gz")

    def device(x, z, y, k):
        return {"gx_0": x, "gx_1": z, "gy": y, "gz": k}

    plane_peers = [
        (n, device((ix + n // NYC) % NXC, iz, (iy + n % NYC) % NYC, ik)) for n in range(1, NXC * NYC)
    ]
    line_peers = [(n, device(ix, (iz + n) % NZC, iy, ik)) for n in range(1, NZC)]
    chain = ix * NZC + iz
    up, down = (chain + 1) % 32, (chain + 31) % 32
    x_peers = [(0, device(up // NZC, up % NZC, iy, ik)), (1, device(down // NZC, down % NZC, iy, ik))]
    y_peers = [
        (n, device(ix, iz, (iy + dy) % NYC, (ik + dk) % 2))
        for n, (dy, dk) in enumerate(((3, 0), (3, 1), (1, 0), (1, 1)))
    ]
    partner = device(ix, iz, iy, 1 - ik)

    def send(src, dst, send_sem, recv_sem, to):
        copy = pltpu.make_async_remote_copy(
            src_ref=src, dst_ref=dst, send_sem=send_sem, recv_sem=recv_sem, device_id=to, device_id_type=MESH
        )
        copy.start()
        return copy

    barrier = pltpu.get_barrier_semaphore()
    greeted = plane_peers + line_peers + x_peers + [y_peers[1], y_peers[3], (0, partner)]
    for _, to in greeted:
        pl.semaphore_signal(barrier, inc=1, device_id=to, device_id_type=MESH)

    for s in range(SLOTS):
        for d in range(2):
            x = F - 1 if d == 0 else 0
            rows = [fine[c, s, x : x + 1, h * 128 : h * 128 + 128] for c in range(3) for h in range(2)]
            tile = jnp.concatenate(rows + [jnp.zeros((2, 128), jnp.float32)], axis=0)
            planes[s * 2 + d] = tile
            planes_in[0, s * 2 + d] = tile
    pl.semaphore_wait(barrier, len(greeted))
    sent = []
    first = [send(other, near_z, y_send.at[4], y_recv.at[4], partner)]
    first += [send(beside.at[n], near_y.at[n], y_send.at[n], y_recv.at[n], to) for n, to in y_peers]
    p_copies = [send(planes, planes_in.at[n], p_send.at[n], p_recv.at[n], to) for n, to in plane_peers]
    for copy in first:
        copy.wait_recv()
    lane = lax.broadcasted_iota(jnp.int32, (1, 128), 1)
    sub = lax.broadcasted_iota(jnp.int32, (8, 128), 0)
    upper = near_y[0] + near_y[1]
    lower = near_y[2] + near_y[3]
    window = []
    for c in range(3):
        cells = own[c] + near_z[c]
        cells += jnp.where((lane >= 90) & (lane < 100), pltpu.roll(upper, 90 - 10 * c, 1), 0.0)
        cells += jnp.where(lane < 10, pltpu.roll(lower, (128 - 10 * c) % 128, 1), 0.0)
        window.append(cells)
        edge[c] = cells[32:40]
    x_copies = [send(edge, edges.at[n], x_send.at[n], x_recv.at[n], to) for n, to in x_peers]

    for copy in p_copies:
        copy.wait_recv()
    pz_copies = []
    for n in range(NZC):
        for j in range(2 * SLOTS):
            at = tab[T_P + n * 8 + j]
            tile = planes_in[at // 8, at % 8]
            if n:
                planes_to[n, j] = tile
            else:
                planes_at[0, j] = tile
        if n:
            pz_copies.append(
                send(planes_to.at[n], planes_at.at[n], pz_send.at[n], pz_recv.at[n], line_peers[n - 1][1])
            )

    for copy in x_copies:
        copy.wait_recv()
    total = jnp.zeros((40, 128), jnp.float32)
    ends = jnp.zeros((8, 128), jnp.float32)
    for c in range(3):
        from_low = jnp.where(chain > 0, edges[0, c], 0.0)
        from_high = jnp.where(chain < 31, edges[1, c], 0.0)
        tile = jnp.where(sub == 0, from_low, jnp.where(sub == 1, from_high, 0.0))
        body = window[c][0:32]
        total += dot(jnp.concatenate([body, tile], axis=0), side[c])
        low = 0.75 * tile[0:1] + 0.25 * body[0:1]
        high = 0.75 * tile[1:2] + 0.25 * body[31:32]
        ends += jnp.where(sub == 2 + 2 * c, low, jnp.where(sub == 3 + 2 * c, high, 0.0))
    total = jnp.concatenate([total[0:32], jnp.where(sub < 2, total[32:40], ends)], axis=0)
    ghost[...] = total
    ghost_in[0] = total
    g_copies = [send(ghost, ghost_in.at[n], g_send.at[n], g_recv.at[n], to) for n, to in plane_peers]
    for copy in g_copies:
        copy.wait_recv()
    gz_copies = []
    for n in range(NZC):
        block = ghost_in[tab[T_D + n]]
        if n:
            ghost_to[n] = block
            gz_copies.append(
                send(ghost_to.at[n], ghost_at.at[n], gz_send.at[n], gz_recv.at[n], line_peers[n - 1][1])
            )
        else:
            ghost_at[0] = block
    for copy in pz_copies + gz_copies:
        copy.wait_recv()

    block = ghost_at[tab[T_OD]]
    lines = dot(along[...], block)
    pulled = dot(lines, spread[...])
    for q in range(SLOTS):
        pull[q] = pulled[q * F : q * F + F]
    faces = dot(block[32:40], face[...])

    lane = lax.broadcasted_iota(jnp.int32, (F, F * F), 1)
    row = lax.broadcasted_iota(jnp.int32, (F, F * F), 0)
    for s in range(SLOTS):
        rate = RATE * visc[s]
        ghosts = pull[tab[T_Q + s]]
        active = tab[T_ACT + s] > 0
        tiles = [planes_at[tab[T_OP + s * 2 + d], s * 2 + d] for d in range(2)]
        near = [tab[T_NEAR + s * 2 + d] > 0 for d in range(2)]
        for c in range(3):
            cells = fine[c, s]
            ends = [
                jnp.where(
                    near[d],
                    jnp.concatenate([tiles[d][2 * c : 2 * c + 1], tiles[d][2 * c + 1 : 2 * c + 2]], axis=1),
                    faces[2 + 2 * c + d : 3 + 2 * c + d],
                )
                for d in range(2)
            ]
            around = ghosts[:, c * F * F : (c + 1) * F * F] - 6.0 * cells
            around += jnp.where(row == 0, ends[0], pltpu.roll(cells, 1, 0))
            around += jnp.where(row == F - 1, ends[1], pltpu.roll(cells, F - 1, 0))
            around += jnp.where(lane < F, 0.0, pltpu.roll(cells, F, 1))
            around += jnp.where(lane >= F * F - F, 0.0, pltpu.roll(cells, F * F - F, 1))
            around += jnp.where(lane % F == 0, 0.0, pltpu.roll(cells, 1, 1))
            around += jnp.where(lane % F == F - 1, 0.0, pltpu.roll(cells, F * F - 1, 1))
            moved = cells + rate * around
            fine_out[c, s] = jnp.where(active, moved, 0.0)
            adv[(c * SLOTS + s) * F : (c * SLOTS + s + 1) * F, :] = moved

    cells = adv[...]
    mean = dot(pair_x[0], dot(cells, pair_yz[0])) + dot(pair_x[1], dot(cells, pair_yz[1]))
    for j in range(6):
        means[j] = mean[j * 8 : j * 8 + 8]
        means_in[0, j] = mean[j * 8 : j * 8 + 8]
    m_copies = [send(means, means_in.at[n], m_send.at[n], m_recv.at[n], to) for n, to in plane_peers]
    for copy in m_copies:
        copy.wait_recv()

    def third(tiles_of, q_low):
        halves = []
        for h in range(2):
            tile, odd = tiles_of(q_low + h)
            flip = (odd == 1) if h == 0 else (odd == 0)
            halves.append(jnp.where(flip, pltpu.roll(tile, 4, 0), tile))
        return jnp.where(sub < 4, halves[0], halves[1])

    mz_copies = []
    for n in range(NZC):
        out = means_to.at[n] if n else means_at.at[0]
        for q in range(SLOTS):
            at = tab[T_V + n * 4 + q]
            out[q] = means_in[at // 4, at % 4]

        def tiles_of(q, n=n):
            at = tab[T_V + n * 4 + q]
            return means_in[at // 4, 4 + at % 4 // 2], at % 2

        for h in range(2):
            out[4 + h] = third(tiles_of, 2 * h)
        if n:
            mz_copies.append(
                send(means_to.at[n], means_at.at[n], mz_send.at[n], mz_recv.at[n], line_peers[n - 1][1])
            )
    for copy in mz_copies:
        copy.wait_recv()
    for q in range(SLOTS):
        boxes[q] = means_at[tab[T_OV + q], q]
    for h in range(2):
        boxes[4 + h] = jnp.where(
            sub < 4, means_at[tab[T_OV + 2 * h], 4 + h], means_at[tab[T_OV + 2 * h + 1], 4 + h]
        )
    for copies in (first, p_copies, x_copies, pz_copies, g_copies, gz_copies, m_copies, mz_copies):
        for copy in copies:
            copy.wait_send()


def place_kernel(tab, boxes, coarse, out, brick, in_sems, out_sems):
    reads = [pltpu.make_async_copy(coarse.at[c], brick.at[c], in_sems.at[c]) for c in range(3)]
    for copy in reads:
        copy.start()
    at = T_WIN + 2 * (6 + 1)
    y, z = tab[at], tab[at + 1]
    shift = z & 127
    here = tab[T_HERE] > 0
    lane = lax.broadcasted_iota(jnp.int32, (8, 128), 1)
    keep = (lane >= shift) & (lane < shift + 8) & here
    y = pl.multiple_of(y, 8)
    z = pl.multiple_of(z - shift, 128)
    writes = []
    for c in range(3):
        reads[c].wait()
        for q in range(SLOTS):
            for a in range(B):
                r = a // 2
                tile, r = (q, c * 4 + r) if c < 2 else (4 + q // 2, q % 2 * 4 + r)
                line = jnp.broadcast_to(boxes[tile, r : r + 1, :], (8, 128))
                line = pltpu.roll(pltpu.roll(line, 72 - 64 * (a % 2), 1, stride=8, stride_axis=0), shift, 1)
                spot = (c, q * B + a, pl.ds(y, 8), pl.ds(z, 128))
                brick[spot] = jnp.where(keep, line, brick[spot])
        copy = pltpu.make_async_copy(brick.at[c], out.at[c], out_sems.at[c])
        copy.start()
        writes.append(copy)
    for copy in writes:
        copy.wait()


def spec(space):
    return pl.BlockSpec(memory_space=space)


def on_device(coarse, fine, visc, corners, grid_slot, neighbors):
    f32 = jnp.float32
    tab = index_table(corners, grid_slot, neighbors)
    own, other, beside = pl.pallas_call(
        window_kernel,
        out_shape=(
            jax.ShapeDtypeStruct((3, 40, 128), f32),
            jax.ShapeDtypeStruct((3, 40, 128), f32),
            jax.ShapeDtypeStruct((4, 40, 128), f32),
        ),
        in_specs=[spec(pltpu.SMEM), spec(pl.ANY)],
        out_specs=(spec(VMEM),) * 3,
        scratch_shapes=[VMEM((2, 3, 32, PITCH, 128), f32), pltpu.SemaphoreType.DMA((2,))],
        name="windows",
    )(tab, coarse)
    dma = pltpu.SemaphoreType.DMA
    n_plane, n_line = NXC * NYC, NZC
    fine_out, boxes = pl.pallas_call(
        exchange_kernel,
        out_shape=(jax.ShapeDtypeStruct(fine.shape, f32), jax.ShapeDtypeStruct((6, 8, 128), f32)),
        in_specs=[spec(pltpu.SMEM)] + [spec(VMEM)] * 11,
        out_specs=(spec(VMEM),) * 2,
        scratch_shapes=[
            VMEM((8, 8, 128), f32),
            VMEM((3, 40, 128), f32),
            VMEM((4, 40, 128), f32),
            VMEM((3, 8, 128), f32),
            VMEM((2, 3, 8, 128), f32),
            VMEM((40, 128), f32),
            VMEM((n_plane, 8, 8, 128), f32),
            VMEM((n_plane, 40, 128), f32),
            VMEM((n_line, 8, 8, 128), f32),
            VMEM((n_line, 40, 128), f32),
            VMEM((n_line, 8, 8, 128), f32),
            VMEM((n_line, 40, 128), f32),
            VMEM((SLOTS, F, 3 * F * F), f32),
            VMEM((3 * SLOTS * F, F * F), f32),
            VMEM((6, 8, 128), f32),
            VMEM((n_plane, 6, 8, 128), f32),
            VMEM((n_line, 6, 8, 128), f32),
            VMEM((n_line, 6, 8, 128), f32),
        ]
        + [dma((5,)), dma((5,)), dma((2,)), dma((2,))]
        + [dma((n_plane,))] * 6
        + [dma((n_line,))] * 6,
        compiler_params=pltpu.CompilerParams(collective_id=1, has_side_effects=True),
        name="exchange",
    )(tab, fine, visc, own, other, beside, *(jnp.asarray(v) for v in constants()))
    coarse_out = pl.pallas_call(
        place_kernel,
        out_shape=jax.ShapeDtypeStruct(coarse.shape, f32),
        in_specs=[spec(pltpu.SMEM), spec(VMEM), spec(pl.ANY)],
        out_specs=spec(pl.ANY),
        scratch_shapes=[VMEM(coarse.shape, f32), dma((3,)), dma((3,))],
        name="place",
    )(tab, boxes, coarse)
    return fine_out, coarse_out


def solution(mesh):
    split = Mesh(
        mesh.devices.reshape(NXC, NZC, mesh.shape["gy"], mesh.shape["gz"]), ("gx_0", "gx_1", "gy", "gz")
    )
    in_specs = (
        P(None, GX, "gy", "gz"),
        P(None, GX_GY_GZ, None, None),
        P(GX_GY_GZ, None, None),
        P(),
        P(),
        P(),
    )
    out_specs = (P(None, GX_GY_GZ, None, None), P(None, GX, "gy", "gz"))
    return jax.shard_map(on_device, mesh=split, in_specs=in_specs, out_specs=out_specs, check_vma=False)
```

```python
import numpy as np
import jax
import jax.numpy as jnp
from jax import lax
from jax.experimental import pallas as pl
from jax.experimental.pallas import tpu as pltpu
from jax.sharding import Mesh
from jax.sharding import PartitionSpec as P

MESH = pl.DeviceIdType.MESH
VMEM = pltpu.VMEM
GX = ("gx_0", "gx_1")
GX_GY_GZ = ("gx_0", "gx_1", "gy", "gz")
B = 8
F = 16
SLOTS = 4
NXC, NZC, NYC = 4, 8, 4
RATE = 0.15
PITCH = 40

T_PLANE = 0
T_GHOST = 1
T_MEAN = 2
T_PLANE_AT = 3
T_GHOST_AT = 4
T_MEAN_AT = 5
T_NEAR = 6
T_ACTIVE = 7
T_BOX = 8
T_HERE = 9
T_Y = 10
T_Z = 11
T_ROWS = 16
LINE, PLANE = NZC, NXC * NYC


def interpolation():
    t = np.zeros((F, B + 2), np.float32)
    for i in range(F):
        center = i // 2 + 1
        t[i, center] += 0.75
        t[i, center - 1 if i % 2 == 0 else center + 1] += 0.25
    return t


def constants():
    t = interpolation()
    low = np.zeros(B + 2, np.float32)
    low[0], low[1] = 0.75, 0.25
    high = low[::-1]
    side = np.zeros((3, 128, 128), np.float32)
    for c in range(3):
        for a in range(B + 2):
            for b in range(B + 2):
                side[c, a * 10 + b, c * 40 + b] += low[a]
                side[c, a * 10 + b, c * 40 + 10 + b] += high[a]
                side[c, a * 10 + b, c * 40 + 20 + a] += low[b]
                side[c, a * 10 + b, c * 40 + 30 + a] += high[b]
    along = np.zeros((SLOTS * F, 40), np.float32)
    for q in range(SLOTS):
        for i in range(F):
            for a in range(B + 2):
                x = 8 * q - 1 + a
                along[q * F + i, 32 if x < 0 else 33 if x > 31 else x] += t[i, a]
    spread = np.zeros((128, 3, F, F), np.float32)
    for c in range(3):
        for u in range(B + 2):
            spread[c * 40 + u, c, 0, :] += t[:, u]
            spread[c * 40 + 10 + u, c, F - 1, :] += t[:, u]
            spread[c * 40 + 20 + u, c, :, 0] += t[:, u]
            spread[c * 40 + 30 + u, c, :, F - 1] += t[:, u]
    face = np.zeros((128, F, F), np.float32)
    face[:100] = np.einsum("ja,lb->abjl", t, t).reshape(100, F, F)
    pair_yz = np.zeros((F, F, 256), np.float32)
    for h in range(2):
        for j in range(F):
            for l in range(F):
                pair_yz[j, l, h * 128 + h * 64 + (7 - j // 2) * 8 + l // 2] = 0.25
    pair_x = np.zeros((2, 2, SLOTS, 8, 3, SLOTS, F), np.float32)
    for part in range(2):
        for h in range(2):
            for s in range(SLOTS):
                for c in range(3):
                    for r in range(2):
                        i = 2 * (2 * (2 * part + r) + h)
                        pair_x[h, part, s, 2 * c + r, c, s, i : i + 2] = 0.5
    return (
        side,
        along,
        spread.reshape(128, 3 * F * F),
        face.reshape(128, F * F),
        pair_yz.reshape(F * F, 256),
        pair_x.reshape(2, 2 * SLOTS * 8, 3 * SLOTS * F),
    )


def index_table(corners, grid_slot, near, ix, iz, iy, ik):
    i32 = jnp.int32
    gs = grid_slot[...]
    cx, cy, cz = corners[0:1], corners[1:2], corners[2:3]
    brick = ((cx >> 5) * NYC + (cy >> 5)) * 2 + (cz >> 8)
    box = (cx >> 3) & 3
    place = (cy & 31) * 256 + (cz & 255)
    total = gs.shape[1]
    grids = lax.broadcasted_iota(i32, (1, total), 1)

    def pick(mask, value):
        return jnp.max(jnp.where(mask, value, -1), axis=1, keepdims=True)

    def lies(n):
        return n >> 6, (n >> 3) & 7, (n >> 1) & 3

    def turn(x, y):
        return ((ix - x) & 3) * NYC + ((iy - y) & 3)

    def block(count, device, side, gather, at):
        n = lax.broadcasted_iota(i32, (count, 1), 0)
        slot = device(n >> 2) * SLOTS + (n & 3)
        own = gs == slot
        beside = pick(own, near[side : side + 1])
        near_slot = jnp.maximum(pick(grids == beside, gs), 0)
        source = jnp.maximum(pick((gs >> 2) == (slot >> 2), brick), 0)
        home = pick(brick * SLOTS + box == slot, gs)
        held = jnp.maximum(home, 0)
        mine = pick(own, box)
        return (
            gather(near_slot >> 2) * SLOTS + (near_slot & 3),
            gather(source),
            gather(held >> 2) * SLOTS + (held & 3),
            at(near_slot >> 2),
            at(source),
            at(held >> 2),
            (beside >= 0).astype(i32),
            (mine >= 0).astype(i32),
            jnp.maximum(mine, 0),
            (home >= 0).astype(i32),
        )

    def plane_gather(d):
        x, z, y = lies(d)
        return jnp.where(z == iz, turn(x, y), 0)

    def line_gather(d):
        x, z, y = lies(d)
        return jnp.where((x == ix) & (y == iy), (iz - z) & 7, 0)

    def line_at(d):
        return (iz - lies(d)[1]) & 7

    def plane_at(d):
        x, _, y = lies(d)
        return turn(x, y)

    along = block(
        LINE * SLOTS,
        lambda o: ((ix * NZC + ((iz + o) & 7)) * NYC + iy) * 2 + ik,
        0, plane_gather, line_at,
    )
    across = block(
        PLANE * SLOTS,
        lambda o: ((((ix + (o >> 2)) & 3) * NZC + iz) * NYC + ((iy + o) & 3)) * 2 + ik,
        1, line_gather, plane_at,
    )
    n = lax.broadcasted_iota(i32, (24, 1), 0)
    x = (ix * NZC + iz + (n & 3) - 1) & 31
    y = (iy + (n >> 3) - 1) & 3
    k = (ik + (n >> 2)) & 1
    found = jnp.maximum(pick((x * NYC + y) * 2 + k == brick, place), 0)
    lane = lax.broadcasted_iota(i32, (1, 128), 1)
    rest = jnp.zeros((128 - 24, 1), i32)
    columns = [jnp.concatenate([a, b, jnp.zeros((32, 1), i32)], axis=0) for a, b in zip(along, across)]
    columns.append(jnp.concatenate([(found >> 8) + (y - iy) * 32, rest], axis=0))
    columns.append(jnp.concatenate([(found & 255) + (k - ik) * 256, rest], axis=0))
    table = jnp.zeros((128, 128), i32)
    for j, column in enumerate(columns):
        table = jnp.where(lane == j, column, table)
    return table.T[0:T_ROWS]


class Window:
    def __init__(self, tab, flat, dy, core, dx):
        at = (dy + 1) * 8 + core * 4 + dx + 1
        self.flat, self.y, self.z = flat, tab[T_Y, at], tab[T_Z, at]
        z = self.z & 255
        self.half, shift = z >> 7, z & 127
        self.first = (shift - 1) & 127
        self.lane = lax.broadcasted_iota(jnp.int32, (1, 128), 1)
        self.cross = ((shift == 0) & (self.lane == 127)) | ((shift == 120) & (self.lane == 0))

    def row(self, c, yy, base, x=None):
        y = self.y - 1 + yy
        inside = (y >= 0) & (y < 32)
        y = jnp.clip(y, 0, 31)

        def take(half):
            start = half * (3 * 32 * PITCH) + c * (32 * PITCH) + y
            if x is None:
                return self.flat[pl.ds(start, 32, stride=PITCH), :]
            return self.flat[pl.ds(start + x * PITCH, 1), :]

        line = jnp.where(self.cross, take(1 - self.half), take(self.half))
        line = pltpu.roll(line, (base - self.first) & 127, 1)
        t = self.lane - base
        z = self.z - 1 + t
        keep = (t >= 0) & (t < 10) & (z >= 0) & (z < 256) & inside
        return jnp.where(keep, line, 0.0)


def parts_of(a):
    first = a.astype(jnp.bfloat16)
    a = a - first.astype(jnp.float32)
    second = a.astype(jnp.bfloat16)
    return first, second, (a - second.astype(jnp.float32)).astype(jnp.bfloat16)


def dot_right(a, weights):
    return sum(jnp.dot(p, weights, preferred_element_type=jnp.float32) for p in parts_of(a))


def dot_left(weights, a):
    return sum(jnp.dot(weights, p, preferred_element_type=jnp.float32) for p in parts_of(a))


def exchange_kernel(
    corners_in, grid_slot_in, near_in, coarse, fine_in, visc_in, side_in, along_in, spread_in, face_in,
    pair_yz_in, pair_x_in,
    result,
    corners, grid_slot, near, fine, visc, side, along, spread, face, pair_yz, pair_x,
    table, tab, brick, own, other, beside, near_z, near_y, edge, edges, pull, adv,
    planes_a, planes_b, ghost_a, ghost_b, means_a, means_b,
    planes_a_in, planes_b_in, ghost_a_in, ghost_b_in, means_a_in, means_b_in,
    planes_a_to, planes_b_to, ghost_a_to, ghost_b_to, means_a_to, means_b_to,
    planes_a_at, planes_b_at, ghost_a_at, ghost_b_at, means_a_at, means_b_at,
    input_sems, local, y_send, y_recv, x_send, x_recv, gather_send, gather_recv, pass_send, pass_recv,
):
    ix, iz = lax.axis_index("gx_0"), lax.axis_index("gx_1")
    iy, ik = lax.axis_index("gy"), lax.axis_index("gz")

    def device(x, z, y, k):
        return {"gx_0": x, "gx_1": z, "gy": y, "gz": k}

    def far(n, count):
        return min(n, count - n)

    plane_peers = [
        (n, device((ix + n // NYC) % NXC, iz, (iy + n % NYC) % NYC, ik))
        for n in sorted(range(1, PLANE), key=lambda n: -far(n // NYC, NXC) - far(n % NYC, NYC))
    ]
    line_peers = [
        (n, device(ix, (iz + n) % NZC, iy, ik)) for n in sorted(range(1, LINE), key=lambda n: -far(n, NZC))
    ]
    chain = ix * NZC + iz
    up, down = (chain + 1) % 32, (chain + 31) % 32
    x_peers = [(0, device(up // NZC, up % NZC, iy, ik)), (1, device(down // NZC, down % NZC, iy, ik))]
    beside_of = ((-1, 0), (-1, 1), (1, 0), (1, 1))
    y_peers = [
        (n, device(ix, iz, (iy + dy) % NYC, (ik + dk) % 2)) for n, (dy, dk) in enumerate(beside_of)
    ]
    partner = device(ix, iz, iy, 1 - ik)
    started = []

    def send(src, dst, send_sem, recv_sem, to):
        copy = pltpu.make_async_remote_copy(
            src_ref=src, dst_ref=dst, send_sem=send_sem, recv_sem=recv_sem, device_id=to, device_id_type=MESH
        )
        copy.start()
        started.append(copy)
        return copy

    def gather(src, dst, peers, item):
        return [
            send(src, dst.at[n], gather_send.at[item, n], gather_recv.at[item, n], to) for n, to in peers
        ]

    def passed(take, to_ref, at_ref, peers, item):
        copies = []
        for n, to in peers:
            take(n, to_ref.at[n])
            copies.append(send(to_ref.at[n], at_ref.at[n], pass_send.at[item, n], pass_recv.at[item, n], to))
        take(0, at_ref.at[0])
        return copies

    def arrive(copies):
        for copy in copies:
            copy.wait_recv()

    loads = [
        pltpu.make_async_copy(
            coarse.at[:, :, :, pl.ds(h * 128, 128)], brick.at[h, :, :, pl.ds(0, 32), :], local.at[h]
        )
        for h in range(2)
    ]
    inputs = [
        pltpu.make_async_copy(src, dst, input_sems.at[n])
        for n, (src, dst) in enumerate(
            (
                (corners_in, corners), (grid_slot_in, grid_slot), (near_in, near), (fine_in, fine),
                (visc_in, visc), (side_in, side), (along_in, along), (spread_in, spread),
                (face_in, face), (pair_yz_in, pair_yz), (pair_x_in, pair_x),
            )
        )
    ]
    for copy in inputs[:4] + loads + inputs[4:]:
        copy.start()
    barrier = pltpu.get_barrier_semaphore()
    greeted = plane_peers + line_peers + x_peers + [y_peers[1], y_peers[3], (0, partner)]
    for _, to in greeted:
        pl.semaphore_signal(barrier, inc=1, device_id=to, device_id_type=MESH)

    for copy in inputs[:3]:
        copy.wait()
    table[...] = index_table(corners, grid_slot, near, ix, iz, iy, ik)
    indices = pltpu.make_async_copy(table, tab, local.at[2])
    indices.start()

    inputs[3].wait()
    for s in range(SLOTS):
        for x, out, out_in in ((F - 1, planes_a, planes_a_in), (0, planes_b, planes_b_in)):
            rows = [fine[c, s, x : x + 1, h * 128 : h * 128 + 128] for c in range(3) for h in range(2)]
            tile = jnp.concatenate(rows, axis=0)
            out[s] = tile
            out_in[0, s] = tile
    pl.semaphore_wait(barrier, len(greeted))
    planes_copies = (
        gather(planes_a, planes_a_in, plane_peers, 0),
        gather(planes_b, planes_b_in, line_peers, 1),
    )

    indices.wait()
    for copy in loads + inputs[4:]:
        copy.wait()
    flat = brick.reshape(2 * 3 * 32 * PITCH, 128)
    lane = lax.broadcasted_iota(jnp.int32, (1, 128), 1)
    sub = lax.broadcasted_iota(jnp.int32, (8, 128), 0)

    def cut(dy, core, rows, out):
        mid, left, right = (Window(tab, flat, dy, core, dx) for dx in (0, -1, 1))
        body = jnp.zeros((32, 128), jnp.float32)
        low = jnp.zeros((1, 128), jnp.float32)
        high = jnp.zeros((1, 128), jnp.float32)
        for c, yy, base in rows:
            body += mid.row(c, yy, base)
            low += right.row(c, yy, base, 31)
            high += left.row(c, yy, base, 0)
        out[0:32, :] = body
        out[32:40, :] = jnp.where(sub == 0, low, jnp.where(sub == 1, high, 0.0))

    first = []
    for n, to in y_peers:
        dy, core = beside_of[n]
        cut(dy, core, [(c, 9 if dy < 0 else 0, c * 10) for c in range(3)], beside.at[n])
        first.append(send(beside.at[n], near_y.at[n], y_send.at[n], y_recv.at[n], to))
    for core, out in ((1, other), (0, own)):
        for c in range(3):
            cut(0, core, [(c, yy, yy * 10) for yy in range(10)], out.at[c])
        if core:
            first.append(send(other, near_z, y_send.at[4], y_recv.at[4], partner))
    arrive(first)
    upper = near_y[0] + near_y[1]
    lower = near_y[2] + near_y[3]
    window = []
    for c in range(3):
        cells = own[c] + near_z[c]
        cells += jnp.where((lane >= 90) & (lane < 100), pltpu.roll(upper, 90 - 10 * c, 1), 0.0)
        cells += jnp.where(lane < 10, pltpu.roll(lower, (128 - 10 * c) % 128, 1), 0.0)
        window.append(cells)
        edge[c] = cells[32:40]
    x_copies = [send(edge, edges.at[n], x_send.at[n], x_recv.at[n], to) for n, to in x_peers]

    def tiles(row, offset, source):
        def take(n, out):
            for s in range(SLOTS):
                at = tab[row, offset + n * SLOTS + s]
                out[s] = source[at // SLOTS, at % SLOTS]

        return take

    def blocks(offset, source):
        def take(n, out):
            out[...] = source[tab[T_GHOST, offset + n * SLOTS]]

        return take

    arrive(planes_copies[0])
    planes_copies += (passed(tiles(T_PLANE, 0, planes_a_in), planes_a_to, planes_a_at, line_peers, 0),)
    arrive(planes_copies[1])
    planes_copies += (passed(tiles(T_PLANE, 32, planes_b_in), planes_b_to, planes_b_at, plane_peers, 1),)

    arrive(x_copies)
    total = jnp.zeros((40, 128), jnp.float32)
    ends = jnp.zeros((8, 128), jnp.float32)
    for c in range(3):
        from_low = jnp.where(chain > 0, edges[0, c], 0.0)
        from_high = jnp.where(chain < 31, edges[1, c], 0.0)
        tile = jnp.where(sub == 0, from_low, jnp.where(sub == 1, from_high, 0.0))
        body = window[c][0:32]
        total += dot_right(jnp.concatenate([body, tile], axis=0), side[c])
        low = 0.75 * tile[0:1] + 0.25 * body[0:1]
        high = 0.75 * tile[1:2] + 0.25 * body[31:32]
        ends += jnp.where(sub == 2 + 2 * c, low, jnp.where(sub == 3 + 2 * c, high, 0.0))
    last = jnp.concatenate([total[24:32], jnp.where(sub < 2, total[32:40], ends)], axis=0)
    ghost_a[...] = total[0:24]
    ghost_a_in[0] = total[0:24]
    ghost_b[...] = last
    ghost_b_in[0] = last
    copies_a = gather(ghost_a, ghost_a_in, plane_peers, 2)
    copies_b = gather(ghost_b, ghost_b_in, line_peers, 3)
    arrive(copies_a)
    ghost_copies = passed(blocks(0, ghost_a_in), ghost_a_to, ghost_a_at, line_peers, 2)
    arrive(copies_b)
    ghost_copies += passed(blocks(32, ghost_b_in), ghost_b_to, ghost_b_at, plane_peers, 3)
    arrive(planes_copies[2])
    arrive(planes_copies[3])
    arrive(ghost_copies)

    block = jnp.concatenate([ghost_a_at[tab[T_GHOST_AT, 0]], ghost_b_at[tab[T_GHOST_AT, 32]]], axis=0)
    pulled = dot_right(dot_left(along[...], block), spread[...])
    for q in range(SLOTS):
        pull[q] = pulled[q * F : q * F + F]
    faces = dot_right(block[32:40], face[...])

    lane = lax.broadcasted_iota(jnp.int32, (F, F * F), 1)
    row = lax.broadcasted_iota(jnp.int32, (F, F * F), 0)
    for s in range(SLOTS):
        rate = RATE * visc[s]
        ghosts = pull[tab[T_BOX, s]]
        active = tab[T_ACTIVE, s] > 0
        planes = (planes_a_at[tab[T_PLANE_AT, s], s], planes_b_at[tab[T_PLANE_AT, 32 + s], s])
        has_near = (tab[T_NEAR, s] > 0, tab[T_NEAR, 32 + s] > 0)
        for c in range(3):
            cells = fine[c, s]
            ends = [
                jnp.where(
                    has_near[d],
                    jnp.concatenate([planes[d][2 * c : 2 * c + 1], planes[d][2 * c + 1 : 2 * c + 2]], axis=1),
                    faces[2 + 2 * c + d : 3 + 2 * c + d],
                )
                for d in range(2)
            ]
            around = ghosts[:, c * F * F : (c + 1) * F * F] - 6.0 * cells
            around += jnp.where(row == 0, ends[0], pltpu.roll(cells, 1, 0))
            around += jnp.where(row == F - 1, ends[1], pltpu.roll(cells, F - 1, 0))
            around += jnp.where(lane < F, 0.0, pltpu.roll(cells, F, 1))
            around += jnp.where(lane >= F * F - F, 0.0, pltpu.roll(cells, F * F - F, 1))
            around += jnp.where(lane % F == 0, 0.0, pltpu.roll(cells, 1, 1))
            around += jnp.where(lane % F == F - 1, 0.0, pltpu.roll(cells, F * F - 1, 1))
            moved = cells + rate * around
            result[c, s] = jnp.where(active, moved, 0.0)
            adv[(c * SLOTS + s) * F : (c * SLOTS + s + 1) * F, :] = moved

    summed = dot_right(adv[...], pair_yz[...])
    mean = dot_left(pair_x[0], summed[:, 0:128]) + dot_left(pair_x[1], summed[:, 128:256])
    for s in range(SLOTS):
        for part, (out, out_in) in enumerate(((means_a, means_a_in), (means_b, means_b_in))):
            tile = mean[part * 32 + s * 8 : part * 32 + s * 8 + 6]
            out[s] = tile
            out_in[0, s] = tile
    facts = (tab[T_Y, 9], tab[T_Z, 9], tab[T_HERE, 0])
    facts = sum(jnp.where(lane[0:1] == n, v.astype(jnp.float32), 0.0) for n, v in enumerate(facts))
    result[2, SLOTS, 0:1, :] = facts
    copies_a = gather(means_a, means_a_in, plane_peers, 4)
    copies_b = gather(means_b, means_b_in, line_peers, 5)
    arrive(copies_a)
    means_copies = passed(tiles(T_MEAN, 0, means_a_in), means_a_to, means_a_at, line_peers, 4)
    arrive(copies_b)
    means_copies += passed(tiles(T_MEAN, 32, means_b_in), means_b_to, means_b_at, plane_peers, 5)
    arrive(means_copies)
    for q in range(SLOTS):
        spot = (SLOTS, slice(q // 2 * 8, q // 2 * 8 + 6), slice(q % 2 * 128, q % 2 * 128 + 128))
        result[0, *spot] = means_a_at[tab[T_MEAN_AT, q], q]
        result[1, *spot] = means_b_at[tab[T_MEAN_AT, 32 + q], q]
    for copy in started:
        copy.wait_send()


def place_kernel(result, coarse, fine_out, out, brick, in_sems, out_sems):
    reads = [pltpu.make_async_copy(coarse.at[c], brick.at[c], in_sems.at[c]) for c in range(3)]
    for copy in reads:
        copy.start()
    writes = [pltpu.make_async_copy(result.at[:, 0:SLOTS], fine_out, out_sems.at[3])]
    writes[0].start()
    lane = lax.broadcasted_iota(jnp.int32, (8, 128), 1)
    facts = result[2, SLOTS, 0:1, 0:128]
    y, z, here = (jnp.sum(jnp.where(lane[0:1] == n, facts, 0.0)).astype(jnp.int32) for n in range(3))
    shift = z & 127
    here = here > 0
    keep = (lane >= shift) & (lane < shift + 8) & here
    y = pl.multiple_of(y, 8)
    z = pl.multiple_of(z - shift, 128)
    for c in range(3):
        reads[c].wait()
        for q in range(SLOTS):
            for a in range(B):
                r = 2 * c + a // 2 % 2
                r += q // 2 * 8
                line = result[a // 4, SLOTS, r : r + 1, q % 2 * 128 : q % 2 * 128 + 128]
                line = jnp.broadcast_to(line, (8, 128))
                line = pltpu.roll(pltpu.roll(line, 72 - 64 * (a % 2), 1, stride=8, stride_axis=0), shift, 1)
                spot = (c, q * B + a, pl.ds(y, 8), pl.ds(z, 128))
                brick[spot] = jnp.where(keep, line, brick[spot])
        copy = pltpu.make_async_copy(brick.at[c], out.at[c], out_sems.at[c])
        copy.start()
        writes.append(copy)
    for copy in writes:
        copy.wait()


def spec(space):
    return pl.BlockSpec(memory_space=space)


def on_device(coarse, fine, visc, corners, grid_slot, neighbors):
    f32 = jnp.float32
    dma = pltpu.SemaphoreType.DMA
    weights = [jnp.asarray(v, jnp.bfloat16) for v in constants()]
    tiles, a, b = (SLOTS, 6, 128), (24, 128), (16, 128)
    sides = (tiles, tiles, a, b, tiles, tiles)
    gathered = [((PLANE, LINE)[n % 2],) + shape for n, shape in enumerate(sides)]
    onward = [((LINE, PLANE)[n % 2],) + shape for n, shape in enumerate(sides)]
    result = pl.pallas_call(
        exchange_kernel,
        out_shape=jax.ShapeDtypeStruct((3, SLOTS + 1, F, F * F), f32),
        in_specs=[spec(pltpu.HBM)] * (6 + len(weights)),
        out_specs=spec(VMEM),
        scratch_shapes=[
            VMEM((3, corners.shape[0]), jnp.int32),
            VMEM((1, corners.shape[0]), jnp.int32),
            VMEM((2, corners.shape[0]), jnp.int32),
            VMEM(fine.shape, f32),
            VMEM(visc.shape, f32),
        ]
        + [VMEM(w.shape, w.dtype) for w in weights]
        + [
            VMEM((T_ROWS, 128), jnp.int32),
            pltpu.SMEM((T_ROWS, 128), jnp.int32),
            VMEM((2, 3, 32, PITCH, 128), f32),
            VMEM((3, 40, 128), f32),
            VMEM((3, 40, 128), f32),
            VMEM((4, 40, 128), f32),
            VMEM((3, 40, 128), f32),
            VMEM((4, 40, 128), f32),
            VMEM((3, 8, 128), f32),
            VMEM((2, 3, 8, 128), f32),
            VMEM((SLOTS, F, 3 * F * F), f32),
            VMEM((3 * SLOTS * F, F * F), f32),
        ]
        + [VMEM(shape, f32) for shape in (*sides, *gathered, *onward, *onward)]
        + [dma((5 + len(weights),)), dma((3,)), dma((5,)), dma((5,)), dma((2,)), dma((2,))]
        + [dma((6, PLANE))] * 4,
        compiler_params=pltpu.CompilerParams(collective_id=1, has_side_effects=True),
        name="exchange",
    )(
        corners.T, grid_slot.reshape(1, -1), neighbors.T, coarse, fine, visc,
        *weights,
    )
    return pl.pallas_call(
        place_kernel,
        out_shape=(jax.ShapeDtypeStruct(fine.shape, f32), jax.ShapeDtypeStruct(coarse.shape, f32)),
        in_specs=[spec(VMEM), spec(pl.ANY)],
        out_specs=(spec(pl.ANY), spec(pl.ANY)),
        scratch_shapes=[VMEM(coarse.shape, f32), dma((3,)), dma((4,))],
        compiler_params=pltpu.CompilerParams(vmem_limit_bytes=16 << 20),
        name="place",
    )(result, coarse)


def solution(mesh):
    split = Mesh(
        mesh.devices.reshape(NXC, NZC, mesh.shape["gy"], mesh.shape["gz"]), ("gx_0", "gx_1", "gy", "gz")
    )
    in_specs = (
        P(None, GX, "gy", "gz"),
        P(None, GX_GY_GZ, None, None),
        P(GX_GY_GZ, None, None),
        P(),
        P(),
        P(),
    )
    out_specs = (P(None, GX_GY_GZ, None, None), P(None, GX, "gy", "gz"))
    return jax.shard_map(on_device, mesh=split, in_specs=in_specs, out_specs=out_specs, check_vma=False)
```

```python
import numpy as np
import jax
import jax.numpy as jnp
from jax import lax
from jax.experimental import pallas as pl
from jax.experimental.pallas import tpu as pltpu
from jax.sharding import Mesh
from jax.sharding import PartitionSpec as P

MESH = pl.DeviceIdType.MESH
VMEM = pltpu.VMEM
GX = ("gx_0", "gx_1")
GX_GY_GZ = ("gx_0", "gx_1", "gy", "gz")
B = 8
F = 16
SLOTS = 4
NXC, NZC, NYC = 4, 8, 4
RATE = 0.15
PITCH = 40

T_PLANE = 0
T_GHOST = 1
T_MEAN = 2
T_PLANE_AT = 3
T_GHOST_AT = 4
T_MEAN_AT = 5
T_NEAR = 6
T_ACTIVE = 7
T_BOX = 8
T_HERE = 9
T_ROWS = 16
W_Y, W_Z = 0, 1
W_ROWS = 8
LINE, PLANE = NZC, NXC * NYC


def interpolation():
    t = np.zeros((F, B + 2), np.float32)
    for i in range(F):
        center = i // 2 + 1
        t[i, center] += 0.75
        t[i, center - 1 if i % 2 == 0 else center + 1] += 0.25
    return t


def constants():
    t = interpolation()
    low = np.zeros(B + 2, np.float32)
    low[0], low[1] = 0.75, 0.25
    high = low[::-1]
    side = np.zeros((3, 128, 128), np.float32)
    for c in range(3):
        for a in range(B + 2):
            for b in range(B + 2):
                side[c, a * 10 + b, c * 40 + b] += low[a]
                side[c, a * 10 + b, c * 40 + 10 + b] += high[a]
                side[c, a * 10 + b, c * 40 + 20 + a] += low[b]
                side[c, a * 10 + b, c * 40 + 30 + a] += high[b]
    along = np.zeros((SLOTS * F, 40), np.float32)
    for q in range(SLOTS):
        for i in range(F):
            for a in range(B + 2):
                x = 8 * q - 1 + a
                along[q * F + i, 32 if x < 0 else 33 if x > 31 else x] += t[i, a]
    spread = np.zeros((128, 3, F, F), np.float32)
    for c in range(3):
        for u in range(B + 2):
            spread[c * 40 + u, c, 0, :] += t[:, u]
            spread[c * 40 + 10 + u, c, F - 1, :] += t[:, u]
            spread[c * 40 + 20 + u, c, :, 0] += t[:, u]
            spread[c * 40 + 30 + u, c, :, F - 1] += t[:, u]
    face = np.zeros((128, F, F), np.float32)
    face[:100] = np.einsum("ja,lb->abjl", t, t).reshape(100, F, F)
    pair_yz = np.zeros((F, F, 256), np.float32)
    for h in range(2):
        for j in range(F):
            for l in range(F):
                pair_yz[j, l, h * 128 + h * 64 + (7 - j // 2) * 8 + l // 2] = 0.25
    pair_x = np.zeros((2, 2, SLOTS, 8, 3, SLOTS, F), np.float32)
    for part in range(2):
        for h in range(2):
            for s in range(SLOTS):
                for c in range(3):
                    for r in range(2):
                        i = 2 * (2 * (2 * part + r) + h)
                        pair_x[h, part, s, 2 * c + r, c, s, i : i + 2] = 0.5
    return (
        side,
        along,
        spread.reshape(128, 3 * F * F),
        face.reshape(128, F * F),
        pair_yz.reshape(F * F, 256),
        pair_x.reshape(2, 2 * SLOTS * 8, 3 * SLOTS * F),
    )


def pick(mask, value):
    return jnp.max(jnp.where(mask, value, -1), axis=1, keepdims=True)


def brick_of(corners):
    return ((corners[0:1] >> 5) * NYC + (corners[1:2] >> 5)) * 2 + (corners[2:3] >> 8)


def as_rows(columns, rows):
    lane = lax.broadcasted_iota(jnp.int32, (1, 128), 1)
    table = jnp.zeros((128, 128), jnp.int32)
    for j, column in enumerate(columns):
        column = jnp.concatenate([column, jnp.zeros((128 - column.shape[0], 1), jnp.int32)], axis=0)
        table = jnp.where(lane == j, column, table)
    return table.T[0:rows]


def window_table(corners, ix, iz, iy, ik):
    place = (corners[1:2] & 31) * 256 + (corners[2:3] & 255)
    n = lax.broadcasted_iota(jnp.int32, (24, 1), 0)
    x = (ix * NZC + iz + (n & 3) - 1) & 31
    y = (iy + (n >> 3) - 1) & 3
    k = (ik + (n >> 2)) & 1
    found = jnp.maximum(pick((x * NYC + y) * 2 + k == brick_of(corners), place), 0)
    return as_rows([(found >> 8) + (y - iy) * 32, (found & 255) + (k - ik) * 256], W_ROWS)


def index_table(corners, grid_slot, near, ix, iz, iy, ik):
    i32 = jnp.int32
    gs = grid_slot[...]
    brick = brick_of(corners)
    box = (corners[0:1] >> 3) & 3
    total = gs.shape[1]
    grids = lax.broadcasted_iota(i32, (1, total), 1)

    def lies(n):
        return n >> 6, (n >> 3) & 7, (n >> 1) & 3

    def turn(x, y):
        return ((ix - x) & 3) * NYC + ((iy - y) & 3)

    def block(count, device, side, gather, at):
        n = lax.broadcasted_iota(i32, (count, 1), 0)
        slot = device(n >> 2) * SLOTS + (n & 3)
        own = gs == slot
        beside = pick(own, near[side : side + 1])
        near_slot = jnp.maximum(pick(grids == beside, gs), 0)
        source = jnp.maximum(pick((gs >> 2) == (slot >> 2), brick), 0)
        home = pick(brick * SLOTS + box == slot, gs)
        held = jnp.maximum(home, 0)
        mine = pick(own, box)
        return (
            gather(near_slot >> 2) * SLOTS + (near_slot & 3),
            gather(source),
            gather(held >> 2) * SLOTS + (held & 3),
            at(near_slot >> 2),
            at(source),
            at(held >> 2),
            (beside >= 0).astype(i32),
            (mine >= 0).astype(i32),
            jnp.maximum(mine, 0),
            (home >= 0).astype(i32),
        )

    def plane_gather(d):
        x, z, y = lies(d)
        return jnp.where(z == iz, turn(x, y), 0)

    def line_gather(d):
        x, z, y = lies(d)
        return jnp.where((x == ix) & (y == iy), (iz - z) & 7, 0)

    def line_at(d):
        return (iz - lies(d)[1]) & 7

    def plane_at(d):
        x, _, y = lies(d)
        return turn(x, y)

    along = block(
        LINE * SLOTS,
        lambda o: ((ix * NZC + ((iz + o) & 7)) * NYC + iy) * 2 + ik,
        0, plane_gather, line_at,
    )
    across = block(
        PLANE * SLOTS,
        lambda o: ((((ix + (o >> 2)) & 3) * NZC + iz) * NYC + ((iy + o) & 3)) * 2 + ik,
        1, line_gather, plane_at,
    )
    return as_rows([jnp.concatenate([a, b], axis=0) for a, b in zip(along, across)], T_ROWS)


class Window:
    def __init__(self, tab, flat, dy, core, dx):
        at = (dy + 1) * 8 + core * 4 + dx + 1
        self.flat, self.y, self.z = flat, tab[W_Y, at], tab[W_Z, at]
        z = self.z & 255
        self.half, shift = z >> 7, z & 127
        self.first = (shift - 1) & 127
        self.lane = lax.broadcasted_iota(jnp.int32, (1, 128), 1)
        self.cross = ((shift == 0) & (self.lane == 127)) | ((shift == 120) & (self.lane == 0))

    def row(self, c, yy, base, x=None):
        y = self.y - 1 + yy
        inside = (y >= 0) & (y < 32)
        y = jnp.clip(y, 0, 31)

        def take(half):
            start = half * (3 * 32 * PITCH) + c * (32 * PITCH) + y
            if x is None:
                return self.flat[pl.ds(start, 32, stride=PITCH), :]
            return self.flat[pl.ds(start + x * PITCH, 1), :]

        line = jnp.where(self.cross, take(1 - self.half), take(self.half))
        line = pltpu.roll(line, (base - self.first) & 127, 1)
        t = self.lane - base
        z = self.z - 1 + t
        keep = (t >= 0) & (t < 10) & (z >= 0) & (z < 256) & inside
        return jnp.where(keep, line, 0.0)


def parts_of(a):
    first = a.astype(jnp.bfloat16)
    a = a - first.astype(jnp.float32)
    second = a.astype(jnp.bfloat16)
    return first, second, (a - second.astype(jnp.float32)).astype(jnp.bfloat16)


def dot_right(a, weights):
    return sum(jnp.dot(p, weights, preferred_element_type=jnp.float32) for p in parts_of(a))


def dot_left(weights, a):
    return sum(jnp.dot(weights, p, preferred_element_type=jnp.float32) for p in parts_of(a))


def exchange_kernel(
    corners_in, grid_slot_in, near_in, coarse, fine_in, visc_in, side_in, along_in, spread_in, face_in,
    pair_yz_in, pair_x_in,
    result,
    corners, grid_slot, near, fine, visc, side, along, spread, face, pair_yz, pair_x,
    table, tab, places, spots, brick, own, other, beside, near_z, near_y, edge, edges, pull, adv,
    planes_a, planes_b, ghost_a, ghost_b, means_a, means_b,
    planes_a_in, planes_b_in, ghost_a_in, ghost_b_in, means_a_in, means_b_in,
    planes_a_to, planes_b_to, ghost_a_to, ghost_b_to, means_a_to, means_b_to,
    planes_a_at, planes_b_at, ghost_a_at, ghost_b_at, means_a_at, means_b_at,
    input_sems, local, y_send, y_recv, x_send, x_recv, gather_send, gather_recv, pass_send, pass_recv,
):
    ix, iz = lax.axis_index("gx_0"), lax.axis_index("gx_1")
    iy, ik = lax.axis_index("gy"), lax.axis_index("gz")

    def device(x, z, y, k):
        return {"gx_0": x, "gx_1": z, "gy": y, "gz": k}

    def far(n, count):
        return min(n, count - n)

    plane_peers = [
        (n, device((ix + n // NYC) % NXC, iz, (iy + n % NYC) % NYC, ik))
        for n in sorted(range(1, PLANE), key=lambda n: -far(n // NYC, NXC) - far(n % NYC, NYC))
    ]
    line_peers = [
        (n, device(ix, (iz + n) % NZC, iy, ik)) for n in sorted(range(1, LINE), key=lambda n: -far(n, NZC))
    ]
    chain = ix * NZC + iz
    beside_of = ((-1, 0), (-1, 1), (1, 0), (1, 1))
    y_peers = [
        (n, device(ix, iz, (iy + dy) % NYC, (ik + dk) % 2)) for n, (dy, dk) in enumerate(beside_of)
    ]
    partner = device(ix, iz, iy, 1 - ik)
    around_of = [(dy, core) for dy in (-1, 1, 0) for core in (0, 1)]
    edge_peers = []
    for side_x, step in enumerate((1, 31)):
        x = (chain + step) % 32
        for n, (dy, core) in enumerate(around_of):
            edge_peers.append(
                (side_x * 6 + n, device(x // NZC, x % NZC, (iy + dy) % NYC, (ik + core) % 2))
            )
    started = []

    def send(src, dst, send_sem, recv_sem, to):
        copy = pltpu.make_async_remote_copy(
            src_ref=src, dst_ref=dst, send_sem=send_sem, recv_sem=recv_sem, device_id=to, device_id_type=MESH
        )
        copy.start()
        started.append(copy)
        return copy

    def gather(src, dst, peers, item):
        return [
            send(src, dst.at[n], gather_send.at[item, n], gather_recv.at[item, n], to) for n, to in peers
        ]

    def passed(take, to_ref, at_ref, peers, item):
        copies = []
        for n, to in peers:
            take(n, to_ref.at[n])
            copies.append(send(to_ref.at[n], at_ref.at[n], pass_send.at[item, n], pass_recv.at[item, n], to))
        take(0, at_ref.at[0])
        return copies

    def arrive(copies):
        for copy in copies:
            copy.wait_recv()

    loads = [
        pltpu.make_async_copy(
            coarse.at[:, :, :, pl.ds(h * 128, 128)], brick.at[h, :, :, pl.ds(0, 32), :], local.at[h]
        )
        for h in range(2)
    ]
    inputs = [
        pltpu.make_async_copy(src, dst, input_sems.at[n])
        for n, (src, dst) in enumerate(
            (
                (corners_in, corners), (grid_slot_in, grid_slot), (near_in, near), (fine_in, fine),
                (visc_in, visc), (side_in, side), (along_in, along), (spread_in, spread),
                (face_in, face), (pair_yz_in, pair_yz), (pair_x_in, pair_x),
            )
        )
    ]
    for copy in inputs[:4] + loads + inputs[4:]:
        copy.start()
    barrier = pltpu.get_barrier_semaphore()
    greeted = plane_peers + line_peers + edge_peers + [y_peers[1], y_peers[3], (0, partner)]
    for _, to in greeted:
        pl.semaphore_signal(barrier, inc=1, device_id=to, device_id_type=MESH)

    inputs[0].wait()
    places[...] = window_table(corners, ix, iz, iy, ik)
    indices = [pltpu.make_async_copy(places, spots, local.at[2]), pltpu.make_async_copy(table, tab, local.at[3])]
    indices[0].start()

    inputs[3].wait()
    for s in range(SLOTS):
        for x, out, out_in in ((F - 1, planes_a, planes_a_in), (0, planes_b, planes_b_in)):
            rows = [fine[c, s, x : x + 1, h * 128 : h * 128 + 128] for c in range(3) for h in range(2)]
            tile = jnp.concatenate(rows, axis=0)
            out[s] = tile
            out_in[0, s] = tile
    pl.semaphore_wait(barrier, len(greeted))
    planes_copies = (
        gather(planes_a, planes_a_in, plane_peers, 0),
        gather(planes_b, planes_b_in, line_peers, 1),
    )

    indices[0].wait()
    for copy in loads + inputs[4:]:
        copy.wait()
    flat = brick.reshape(2 * 3 * 32 * PITCH, 128)
    lane = lax.broadcasted_iota(jnp.int32, (1, 128), 1)
    sub = lax.broadcasted_iota(jnp.int32, (8, 128), 0)

    def cut(dy, core, rows, out):
        mid = Window(spots, flat, dy, core, 0)
        out[...] = sum(mid.row(c, yy, base) for c, yy, base in rows)

    def cut_edges(n, dy, core):
        for side_x, x in enumerate((31, 0)):
            window = Window(spots, flat, dy, core, 1 - 2 * side_x)
            tile = jnp.zeros((8, 128), jnp.float32)
            for c in range(3):
                lines = [(9,), (0,), range(10)][(-1, 1, 0).index(dy)]
                line = sum(window.row(c, yy, yy * 10, x) for yy in lines)
                tile = jnp.where(sub == c, line, tile)
            edge[side_x * 6 + n] = tile

    first = []
    for n, to in y_peers:
        dy, core = beside_of[n]
        cut(dy, core, [(c, 9 if dy < 0 else 0, c * 10) for c in range(3)], beside.at[n])
        first.append(send(beside.at[n], near_y.at[n], y_send.at[n], y_recv.at[n], to))
    for n, (dy, core) in enumerate(around_of):
        cut_edges(n, dy, core)
        for at in (n, 6 + n):
            first.append(send(edge.at[at], edges.at[at], x_send.at[at], x_recv.at[at], edge_peers[at][1]))
    for core, out in ((1, other), (0, own)):
        for c in range(3):
            cut(0, core, [(c, yy, yy * 10) for yy in range(10)], out.at[c])
        if core:
            first.append(send(other, near_z, y_send.at[4], y_recv.at[4], partner))
    for copy in inputs[1:3]:
        copy.wait()
    table[...] = index_table(corners, grid_slot, near, ix, iz, iy, ik)
    indices[1].start()
    arrive(first)
    upper = near_y[0] + near_y[1]
    lower = near_y[2] + near_y[3]
    from_low = jnp.where(chain > 0, sum(edges[n] for n in range(6)), 0.0)
    from_high = jnp.where(chain < 31, sum(edges[n] for n in range(6, 12)), 0.0)
    total = jnp.zeros((40, 128), jnp.float32)
    ends = jnp.zeros((8, 128), jnp.float32)
    for c in range(3):
        body = own[c] + near_z[c]
        body += jnp.where((lane >= 90) & (lane < 100), pltpu.roll(upper, 90 - 10 * c, 1), 0.0)
        body += jnp.where(lane < 10, pltpu.roll(lower, (128 - 10 * c) % 128, 1), 0.0)
        low, high = from_low[c : c + 1], from_high[c : c + 1]
        tile = jnp.where(sub == 0, low, jnp.where(sub == 1, high, 0.0))
        total += dot_right(jnp.concatenate([body, tile], axis=0), side[c])
        low = 0.75 * low + 0.25 * body[0:1]
        high = 0.75 * high + 0.25 * body[31:32]
        ends += jnp.where(sub == 2 + 2 * c, low, jnp.where(sub == 3 + 2 * c, high, 0.0))
    last = jnp.concatenate([total[24:32], jnp.where(sub < 2, total[32:40], ends)], axis=0)
    ghost_a[...] = total[0:24]
    ghost_a_in[0] = total[0:24]
    ghost_b[...] = last
    ghost_b_in[0] = last
    copies_a = gather(ghost_a, ghost_a_in, plane_peers, 2)
    copies_b = gather(ghost_b, ghost_b_in, line_peers, 3)
    indices[1].wait()

    def tiles(row, offset, source):
        def take(n, out):
            for s in range(SLOTS):
                at = tab[row, offset + n * SLOTS + s]
                out[s] = source[at // SLOTS, at % SLOTS]

        return take

    def blocks(offset, source):
        def take(n, out):
            out[...] = source[tab[T_GHOST, offset + n * SLOTS]]

        return take

    arrive(planes_copies[0])
    planes_copies += (passed(tiles(T_PLANE, 0, planes_a_in), planes_a_to, planes_a_at, line_peers, 0),)
    arrive(planes_copies[1])
    planes_copies += (passed(tiles(T_PLANE, 32, planes_b_in), planes_b_to, planes_b_at, plane_peers, 1),)

    arrive(copies_a)
    ghost_copies = passed(blocks(0, ghost_a_in), ghost_a_to, ghost_a_at, line_peers, 2)
    arrive(copies_b)
    ghost_copies += passed(blocks(32, ghost_b_in), ghost_b_to, ghost_b_at, plane_peers, 3)
    arrive(planes_copies[2])
    arrive(planes_copies[3])
    arrive(ghost_copies)

    block = jnp.concatenate([ghost_a_at[tab[T_GHOST_AT, 0]], ghost_b_at[tab[T_GHOST_AT, 32]]], axis=0)
    pulled = dot_right(dot_left(along[...], block), spread[...])
    for q in range(SLOTS):
        pull[q] = pulled[q * F : q * F + F]
    faces = dot_right(block[32:40], face[...])

    lane = lax.broadcasted_iota(jnp.int32, (F, F * F), 1)
    row = lax.broadcasted_iota(jnp.int32, (F, F * F), 0)
    for s in range(SLOTS):
        rate = RATE * visc[s]
        ghosts = pull[tab[T_BOX, s]]
        active = tab[T_ACTIVE, s] > 0
        planes = (planes_a_at[tab[T_PLANE_AT, s], s], planes_b_at[tab[T_PLANE_AT, 32 + s], s])
        has_near = (tab[T_NEAR, s] > 0, tab[T_NEAR, 32 + s] > 0)
        for c in range(3):
            cells = fine[c, s]
            ends = [
                jnp.where(
                    has_near[d],
                    jnp.concatenate([planes[d][2 * c : 2 * c + 1], planes[d][2 * c + 1 : 2 * c + 2]], axis=1),
                    faces[2 + 2 * c + d : 3 + 2 * c + d],
                )
                for d in range(2)
            ]
            around = ghosts[:, c * F * F : (c + 1) * F * F] - 6.0 * cells
            around += jnp.where(row == 0, ends[0], pltpu.roll(cells, 1, 0))
            around += jnp.where(row == F - 1, ends[1], pltpu.roll(cells, F - 1, 0))
            around += jnp.where(lane < F, 0.0, pltpu.roll(cells, F, 1))
            around += jnp.where(lane >= F * F - F, 0.0, pltpu.roll(cells, F * F - F, 1))
            around += jnp.where(lane % F == 0, 0.0, pltpu.roll(cells, 1, 1))
            around += jnp.where(lane % F == F - 1, 0.0, pltpu.roll(cells, F * F - 1, 1))
            moved = cells + rate * around
            result[c, s] = jnp.where(active, moved, 0.0)
            adv[(c * SLOTS + s) * F : (c * SLOTS + s + 1) * F, :] = moved

    summed = dot_right(adv[...], pair_yz[...])
    mean = dot_left(pair_x[0], summed[:, 0:128]) + dot_left(pair_x[1], summed[:, 128:256])
    for s in range(SLOTS):
        for part, (out, out_in) in enumerate(((means_a, means_a_in), (means_b, means_b_in))):
            tile = mean[part * 32 + s * 8 : part * 32 + s * 8 + 6]
            out[s] = tile
            out_in[0, s] = tile
    facts = (spots[W_Y, 9], spots[W_Z, 9], tab[T_HERE, 0])
    facts = sum(jnp.where(lane[0:1] == n, v.astype(jnp.float32), 0.0) for n, v in enumerate(facts))
    result[2, SLOTS, 0:1, :] = facts
    copies_a = gather(means_a, means_a_in, plane_peers, 4)
    copies_b = gather(means_b, means_b_in, line_peers, 5)
    arrive(copies_a)
    means_copies = passed(tiles(T_MEAN, 0, means_a_in), means_a_to, means_a_at, line_peers, 4)
    arrive(copies_b)
    means_copies += passed(tiles(T_MEAN, 32, means_b_in), means_b_to, means_b_at, plane_peers, 5)
    arrive(means_copies)
    for q in range(SLOTS):
        spot = (SLOTS, slice(q // 2 * 8, q // 2 * 8 + 6), slice(q % 2 * 128, q % 2 * 128 + 128))
        result[0, *spot] = means_a_at[tab[T_MEAN_AT, q], q]
        result[1, *spot] = means_b_at[tab[T_MEAN_AT, 32 + q], q]
    for copy in started:
        copy.wait_send()


def place_kernel(result, coarse, fine_out, out, brick, in_sems, out_sems):
    reads = [pltpu.make_async_copy(coarse.at[c], brick.at[c], in_sems.at[c]) for c in range(3)]
    for copy in reads:
        copy.start()
    writes = [pltpu.make_async_copy(result.at[:, 0:SLOTS], fine_out, out_sems.at[3])]
    writes[0].start()
    lane = lax.broadcasted_iota(jnp.int32, (8, 128), 1)
    facts = result[2, SLOTS, 0:1, 0:128]
    y, z, here = (jnp.sum(jnp.where(lane[0:1] == n, facts, 0.0)).astype(jnp.int32) for n in range(3))
    shift = z & 127
    here = here > 0
    keep = (lane >= shift) & (lane < shift + 8) & here
    y = pl.multiple_of(y, 8)
    z = pl.multiple_of(z - shift, 128)
    for c in range(3):
        reads[c].wait()
        for q in range(SLOTS):
            for a in range(B):
                r = 2 * c + a // 2 % 2
                r += q // 2 * 8
                line = result[a // 4, SLOTS, r : r + 1, q % 2 * 128 : q % 2 * 128 + 128]
                line = jnp.broadcast_to(line, (8, 128))
                line = pltpu.roll(pltpu.roll(line, 72 - 64 * (a % 2), 1, stride=8, stride_axis=0), shift, 1)
                spot = (c, q * B + a, pl.ds(y, 8), pl.ds(z, 128))
                brick[spot] = jnp.where(keep, line, brick[spot])
        copy = pltpu.make_async_copy(brick.at[c], out.at[c], out_sems.at[c])
        copy.start()
        writes.append(copy)
    for copy in writes:
        copy.wait()


def spec(space):
    return pl.BlockSpec(memory_space=space)


def on_device(coarse, fine, visc, corners, grid_slot, neighbors):
    f32 = jnp.float32
    dma = pltpu.SemaphoreType.DMA
    weights = [jnp.asarray(v, jnp.bfloat16) for v in constants()]
    tiles, a, b = (SLOTS, 6, 128), (24, 128), (16, 128)
    sides = (tiles, tiles, a, b, tiles, tiles)
    gathered = [((PLANE, LINE)[n % 2],) + shape for n, shape in enumerate(sides)]
    onward = [((LINE, PLANE)[n % 2],) + shape for n, shape in enumerate(sides)]
    result = pl.pallas_call(
        exchange_kernel,
        out_shape=jax.ShapeDtypeStruct((3, SLOTS + 1, F, F * F), f32),
        in_specs=[spec(pltpu.HBM)] * (6 + len(weights)),
        out_specs=spec(VMEM),
        scratch_shapes=[
            VMEM((3, corners.shape[0]), jnp.int32),
            VMEM((1, corners.shape[0]), jnp.int32),
            VMEM((2, corners.shape[0]), jnp.int32),
            VMEM(fine.shape, f32),
            VMEM(visc.shape, f32),
        ]
        + [VMEM(w.shape, w.dtype) for w in weights]
        + [
            VMEM((T_ROWS, 128), jnp.int32),
            pltpu.SMEM((T_ROWS, 128), jnp.int32),
            VMEM((W_ROWS, 128), jnp.int32),
            pltpu.SMEM((W_ROWS, 128), jnp.int32),
            VMEM((2, 3, 32, PITCH, 128), f32),
            VMEM((3, 32, 128), f32),
            VMEM((3, 32, 128), f32),
            VMEM((4, 32, 128), f32),
            VMEM((3, 32, 128), f32),
            VMEM((4, 32, 128), f32),
            VMEM((12, 8, 128), f32),
            VMEM((12, 8, 128), f32),
            VMEM((SLOTS, F, 3 * F * F), f32),
            VMEM((3 * SLOTS * F, F * F), f32),
        ]
        + [VMEM(shape, f32) for shape in (*sides, *gathered, *onward, *onward)]
        + [dma((5 + len(weights),)), dma((4,)), dma((5,)), dma((5,)), dma((12,)), dma((12,))]
        + [dma((6, PLANE))] * 4,
        compiler_params=pltpu.CompilerParams(collective_id=1, has_side_effects=True),
        name="exchange",
    )(
        corners.T, grid_slot.reshape(1, -1), neighbors.T, coarse, fine, visc,
        *weights,
    )
    return pl.pallas_call(
        place_kernel,
        out_shape=(jax.ShapeDtypeStruct(fine.shape, f32), jax.ShapeDtypeStruct(coarse.shape, f32)),
        in_specs=[spec(VMEM), spec(pl.ANY)],
        out_specs=(spec(pl.ANY), spec(pl.ANY)),
        scratch_shapes=[VMEM(coarse.shape, f32), dma((3,)), dma((4,))],
        compiler_params=pltpu.CompilerParams(vmem_limit_bytes=16 << 20),
        name="place",
    )(result, coarse)


def solution(mesh):
    split = Mesh(
        mesh.devices.reshape(NXC, NZC, mesh.shape["gy"], mesh.shape["gz"]), ("gx_0", "gx_1", "gy", "gz")
    )
    in_specs = (
        P(None, GX, "gy", "gz"),
        P(None, GX_GY_GZ, None, None),
        P(GX_GY_GZ, None, None),
        P(),
        P(),
        P(),
    )
    out_specs = (P(None, GX_GY_GZ, None, None), P(None, GX, "gy", "gz"))
    return jax.shard_map(on_device, mesh=split, in_specs=in_specs, out_specs=out_specs, check_vma=False)
```

```python
import numpy as np
import jax
import jax.numpy as jnp
from jax import lax
from jax.experimental import pallas as pl
from jax.experimental.pallas import tpu as pltpu
from jax.sharding import Mesh
from jax.sharding import PartitionSpec as P

MESH = pl.DeviceIdType.MESH
VMEM = pltpu.VMEM
GX = ("gx_0", "gx_1")
GX_GY_GZ = ("gx_0", "gx_1", "gy", "gz")
B = 8
F = 16
SLOTS = 4
NXC, NZC, NYC = 4, 8, 4
RATE = 0.15
PITCH = 40

T_PLANE = 0
T_GHOST = 1
T_MEAN = 2
T_PLANE_AT = 3
T_GHOST_AT = 4
T_MEAN_AT = 5
T_NEAR = 6
T_ACTIVE = 7
T_BOX = 8
T_HERE = 9
T_ROWS = 16
W_Y, W_Z = 0, 1
W_ROWS = 8
LINE, PLANE = NZC, NXC * NYC


def interpolation():
    t = np.zeros((F, B + 2), np.float32)
    for i in range(F):
        center = i // 2 + 1
        t[i, center] += 0.75
        t[i, center - 1 if i % 2 == 0 else center + 1] += 0.25
    return t


def constants():
    t = interpolation()
    low = np.zeros(B + 2, np.float32)
    low[0], low[1] = 0.75, 0.25
    high = low[::-1]
    side = np.zeros((3, 128, 128), np.float32)
    for c in range(3):
        for a in range(B + 2):
            for b in range(B + 2):
                side[c, a * 10 + b, c * 40 + b] += low[a]
                side[c, a * 10 + b, c * 40 + 10 + b] += high[a]
                side[c, a * 10 + b, c * 40 + 20 + a] += low[b]
                side[c, a * 10 + b, c * 40 + 30 + a] += high[b]
    along = np.zeros((SLOTS * F, 40), np.float32)
    for q in range(SLOTS):
        for i in range(F):
            for a in range(B + 2):
                x = 8 * q - 1 + a
                along[q * F + i, 32 if x < 0 else 33 if x > 31 else x] += t[i, a]
    spread = np.zeros((128, 3, F, F), np.float32)
    for c in range(3):
        for u in range(B + 2):
            spread[c * 40 + u, c, 0, :] += t[:, u]
            spread[c * 40 + 10 + u, c, F - 1, :] += t[:, u]
            spread[c * 40 + 20 + u, c, :, 0] += t[:, u]
            spread[c * 40 + 30 + u, c, :, F - 1] += t[:, u]
    face = np.zeros((128, F, F), np.float32)
    face[:100] = np.einsum("ja,lb->abjl", t, t).reshape(100, F, F)
    pair_yz = np.zeros((F, F, 256), np.float32)
    for h in range(2):
        for j in range(F):
            for l in range(F):
                pair_yz[j, l, h * 128 + h * 64 + (7 - j // 2) * 8 + l // 2] = 0.25
    pair_x = np.zeros((2, 2, SLOTS, 8, 3, SLOTS, F), np.float32)
    for part in range(2):
        for h in range(2):
            for s in range(SLOTS):
                for c in range(3):
                    for r in range(2):
                        i = 2 * (2 * (2 * part + r) + h)
                        pair_x[h, part, s, 2 * c + r, c, s, i : i + 2] = 0.5
    return (
        side,
        along,
        spread.reshape(128, 3 * F * F),
        face.reshape(128, F * F),
        pair_yz.reshape(F * F, 256),
        pair_x.reshape(2, 2 * SLOTS * 8, 3 * SLOTS * F),
    )


def pick(mask, value):
    return jnp.max(jnp.where(mask, value, -1), axis=1, keepdims=True)


def brick_of(corners):
    return ((corners[0:1] >> 5) * NYC + (corners[1:2] >> 5)) * 2 + (corners[2:3] >> 8)


def as_rows(columns, rows):
    lane = lax.broadcasted_iota(jnp.int32, (1, 128), 1)
    table = jnp.zeros((128, 128), jnp.int32)
    for j, column in enumerate(columns):
        column = jnp.concatenate([column, jnp.zeros((128 - column.shape[0], 1), jnp.int32)], axis=0)
        table = jnp.where(lane == j, column, table)
    return table.T[0:rows]


def window_table(corners, ix, iz, iy, ik):
    place = (corners[1:2] & 31) * 256 + (corners[2:3] & 255)
    n = lax.broadcasted_iota(jnp.int32, (24, 1), 0)
    x = (ix * NZC + iz + (n & 3) - 1) & 31
    y = (iy + (n >> 3) - 1) & 3
    k = (ik + (n >> 2)) & 1
    found = jnp.maximum(pick((x * NYC + y) * 2 + k == brick_of(corners), place), 0)
    return as_rows([(found >> 8) + (y - iy) * 32, (found & 255) + (k - ik) * 256], W_ROWS)


def index_table(corners, grid_slot, near, ix, iz, iy, ik):
    i32 = jnp.int32
    gs = grid_slot[...]
    brick = brick_of(corners)
    box = (corners[0:1] >> 3) & 3
    total = gs.shape[1]
    grids = lax.broadcasted_iota(i32, (1, total), 1)

    def lies(n):
        return n >> 6, (n >> 3) & 7, (n >> 1) & 3

    def turn(x, y):
        return ((ix - x) & 3) * NYC + ((iy - y) & 3)

    def block(count, device, side, gather, at):
        n = lax.broadcasted_iota(i32, (count, 1), 0)
        slot = device(n >> 2) * SLOTS + (n & 3)
        own = gs == slot
        beside = pick(own, near[side : side + 1])
        near_slot = jnp.maximum(pick(grids == beside, gs), 0)
        source = jnp.maximum(pick((gs >> 2) == (slot >> 2), brick), 0)
        home = pick(brick * SLOTS + box == slot, gs)
        held = jnp.maximum(home, 0)
        mine = pick(own, box)
        return (
            gather(near_slot >> 2) * SLOTS + (near_slot & 3),
            gather(source),
            gather(held >> 2) * SLOTS + (held & 3),
            at(near_slot >> 2),
            at(source),
            at(held >> 2),
            (beside >= 0).astype(i32),
            (mine >= 0).astype(i32),
            jnp.maximum(mine, 0),
            (home >= 0).astype(i32),
        )

    def plane_gather(d):
        x, z, y = lies(d)
        return jnp.where(z == iz, turn(x, y), 0)

    def line_gather(d):
        x, z, y = lies(d)
        return jnp.where((x == ix) & (y == iy), (iz - z) & 7, 0)

    def line_at(d):
        return (iz - lies(d)[1]) & 7

    def plane_at(d):
        x, _, y = lies(d)
        return turn(x, y)

    along = block(
        LINE * SLOTS,
        lambda o: ((ix * NZC + ((iz + o) & 7)) * NYC + iy) * 2 + ik,
        0, plane_gather, line_at,
    )
    across = block(
        PLANE * SLOTS,
        lambda o: ((((ix + (o >> 2)) & 3) * NZC + iz) * NYC + ((iy + o) & 3)) * 2 + ik,
        1, line_gather, plane_at,
    )
    return as_rows([jnp.concatenate([a, b], axis=0) for a, b in zip(along, across)], T_ROWS)


class Window:
    def __init__(self, tab, flat, dy, core, dx):
        at = (dy + 1) * 8 + core * 4 + dx + 1
        self.flat, self.y, self.z = flat, tab[W_Y, at], tab[W_Z, at]
        z = self.z & 255
        self.half, shift = z >> 7, z & 127
        self.first = (shift - 1) & 127
        self.lane = lax.broadcasted_iota(jnp.int32, (1, 128), 1)
        self.cross = ((shift == 0) & (self.lane == 127)) | ((shift == 120) & (self.lane == 0))

    def row(self, c, yy, base, x=None):
        y = self.y - 1 + yy
        inside = (y >= 0) & (y < 32)
        y = jnp.clip(y, 0, 31)

        def take(half):
            start = half * (3 * 32 * PITCH) + c * (32 * PITCH) + y
            if x is None:
                return self.flat[pl.ds(start, 32, stride=PITCH), :]
            return self.flat[pl.ds(start + x * PITCH, 1), :]

        line = jnp.where(self.cross, take(1 - self.half), take(self.half))
        line = pltpu.roll(line, (base - self.first) & 127, 1)
        t = self.lane - base
        z = self.z - 1 + t
        keep = (t >= 0) & (t < 10) & (z >= 0) & (z < 256) & inside
        return jnp.where(keep, line, 0.0)


def parts_of(a):
    first = a.astype(jnp.bfloat16)
    a = a - first.astype(jnp.float32)
    second = a.astype(jnp.bfloat16)
    return first, second, (a - second.astype(jnp.float32)).astype(jnp.bfloat16)


def dot_right(a, weights):
    return sum(jnp.dot(p, weights, preferred_element_type=jnp.float32) for p in parts_of(a))


def dot_left(weights, a):
    return sum(jnp.dot(weights, p, preferred_element_type=jnp.float32) for p in parts_of(a))


def exchange_kernel(
    corners_in, grid_slot_in, near_in, coarse, fine_in, visc_in, side_in, along_in, spread_in, face_in,
    pair_yz_in, pair_x_in,
    result,
    corners, grid_slot, near, fine, visc, side, along, spread, face, pair_yz, pair_x,
    table, tab, places, spots, brick, own, other, beside, near_z, near_y, edge, edges, pull, adv,
    planes_a, planes_b, ghost_a, ghost_b, means_a, means_b,
    planes_a_in, planes_b_in, ghost_a_in, ghost_b_in, means_a_in, means_b_in,
    planes_a_to, planes_b_to, ghost_a_to, ghost_b_to, means_a_to, means_b_to,
    planes_a_at, planes_b_at, ghost_a_at, ghost_b_at, means_a_at, means_b_at,
    input_sems, local, y_send, y_recv, x_send, x_recv, gather_send, gather_recv, pass_send, pass_recv,
):
    ix, iz = lax.axis_index("gx_0"), lax.axis_index("gx_1")
    iy, ik = lax.axis_index("gy"), lax.axis_index("gz")

    def device(x, z, y, k):
        return {"gx_0": x, "gx_1": z, "gy": y, "gz": k}

    def far(n, count):
        return min(n, count - n)

    plane_peers = [
        (n, device(lax.rem(ix + n // NYC, NXC), iz, lax.rem(iy + n % NYC, NYC), ik))
        for n in sorted(range(1, PLANE), key=lambda n: -far(n // NYC, NXC) - far(n % NYC, NYC))
    ]
    line_peers = [
        (n, device(ix, lax.rem(iz + n, NZC), iy, ik)) for n in sorted(range(1, LINE), key=lambda n: -far(n, NZC))
    ]
    chain = ix * NZC + iz
    beside_of = ((-1, 0), (-1, 1), (1, 0), (1, 1))
    y_peers = [
        (n, device(ix, iz, lax.rem(iy + NYC + dy, NYC), lax.rem(ik + dk, 2))) for n, (dy, dk) in enumerate(beside_of)
    ]
    partner = device(ix, iz, iy, 1 - ik)
    around_of = [(dy, core) for dy in (-1, 1, 0) for core in (0, 1)]
    edge_peers = []
    for side_x, step in enumerate((1, 31)):
        x = lax.rem(chain + step, 32)
        for n, (dy, core) in enumerate(around_of):
            edge_peers.append(
                (side_x * 6 + n, device(lax.div(x, NZC), lax.rem(x, NZC), lax.rem(iy + NYC + dy, NYC), lax.rem(ik + core, 2)))
            )
    started = []

    def send(src, dst, send_sem, recv_sem, to):
        copy = pltpu.make_async_remote_copy(
            src_ref=src, dst_ref=dst, send_sem=send_sem, recv_sem=recv_sem, device_id=to, device_id_type=MESH
        )
        copy.start()
        started.append(copy)
        return copy

    def gather(src, dst, peers, item):
        return [
            send(src, dst.at[n], gather_send.at[item, n], gather_recv.at[item, n], to) for n, to in peers
        ]

    def passed(take, to_ref, at_ref, peers, item):
        copies = []
        for n, to in peers:
            take(n, to_ref.at[n])
            copies.append(send(to_ref.at[n], at_ref.at[n], pass_send.at[item, n], pass_recv.at[item, n], to))
        take(0, at_ref.at[0])
        return copies

    def arrive(copies):
        for copy in copies:
            copy.wait_recv()

    loads = [
        pltpu.make_async_copy(
            coarse.at[:, :, :, pl.ds(h * 128, 128)], brick.at[h, :, :, pl.ds(0, 32), :], local.at[h]
        )
        for h in range(2)
    ]
    inputs = [
        pltpu.make_async_copy(src, dst, input_sems.at[n])
        for n, (src, dst) in enumerate(
            (
                (corners_in, corners), (grid_slot_in, grid_slot), (near_in, near), (fine_in, fine),
                (visc_in, visc), (side_in, side), (along_in, along), (spread_in, spread),
                (face_in, face), (pair_yz_in, pair_yz), (pair_x_in, pair_x),
            )
        )
    ]
    for copy in inputs[:4] + loads + inputs[4:]:
        copy.start()
    barrier = pltpu.get_barrier_semaphore()
    greeted = plane_peers + line_peers + edge_peers + [y_peers[1], y_peers[3], (0, partner)]
    for _, to in greeted:
        pl.semaphore_signal(barrier, inc=1, device_id=to, device_id_type=MESH)

    inputs[0].wait()
    places[...] = window_table(corners, ix, iz, iy, ik)
    indices = [pltpu.make_async_copy(places, spots, local.at[2]), pltpu.make_async_copy(table, tab, local.at[3])]
    indices[0].start()

    inputs[3].wait()
    for s in range(SLOTS):
        for x, out, out_in in ((F - 1, planes_a, planes_a_in), (0, planes_b, planes_b_in)):
            rows = [fine[c, s, x : x + 1, h * 128 : h * 128 + 128] for c in range(3) for h in range(2)]
            tile = jnp.concatenate(rows, axis=0)
            out[s] = tile
            out_in[0, s] = tile
    pl.semaphore_wait(barrier, len(greeted))
    planes_copies = (
        gather(planes_a, planes_a_in, plane_peers, 0),
        gather(planes_b, planes_b_in, line_peers, 1),
    )

    indices[0].wait()
    for copy in loads + inputs[4:]:
        copy.wait()
    flat = brick.reshape(2 * 3 * 32 * PITCH, 128)
    lane = lax.broadcasted_iota(jnp.int32, (1, 128), 1)
    sub = lax.broadcasted_iota(jnp.int32, (8, 128), 0)

    def cut(dy, core, rows, out):
        mid = Window(spots, flat, dy, core, 0)
        out[...] = sum(mid.row(c, yy, base) for c, yy, base in rows)

    def cut_edges(n, dy, core):
        for side_x, x in enumerate((31, 0)):
            window = Window(spots, flat, dy, core, 1 - 2 * side_x)
            tile = jnp.zeros((8, 128), jnp.float32)
            for c in range(3):
                lines = [(9,), (0,), range(10)][(-1, 1, 0).index(dy)]
                line = sum(window.row(c, yy, yy * 10, x) for yy in lines)
                tile = jnp.where(sub == c, line, tile)
            edge[side_x * 6 + n] = tile

    first = []
    for n, to in y_peers:
        dy, core = beside_of[n]
        cut(dy, core, [(c, 9 if dy < 0 else 0, c * 10) for c in range(3)], beside.at[n])
        first.append(send(beside.at[n], near_y.at[n], y_send.at[n], y_recv.at[n], to))
    for n, (dy, core) in enumerate(around_of):
        cut_edges(n, dy, core)
        for at in (n, 6 + n):
            first.append(send(edge.at[at], edges.at[at], x_send.at[at], x_recv.at[at], edge_peers[at][1]))
    for core, out in ((1, other), (0, own)):
        for c in range(3):
            cut(0, core, [(c, yy, yy * 10) for yy in range(10)], out.at[c])
        if core:
            first.append(send(other, near_z, y_send.at[4], y_recv.at[4], partner))
    for copy in inputs[1:3]:
        copy.wait()
    table[...] = index_table(corners, grid_slot, near, ix, iz, iy, ik)
    indices[1].start()
    arrive(first)
    upper = near_y[0] + near_y[1]
    lower = near_y[2] + near_y[3]
    from_low = jnp.where(chain > 0, sum(edges[n] for n in range(6)), 0.0)
    from_high = jnp.where(chain < 31, sum(edges[n] for n in range(6, 12)), 0.0)
    total = jnp.zeros((40, 128), jnp.float32)
    ends = jnp.zeros((8, 128), jnp.float32)
    for c in range(3):
        body = own[c] + near_z[c]
        body += jnp.where((lane >= 90) & (lane < 100), pltpu.roll(upper, 90 - 10 * c, 1), 0.0)
        body += jnp.where(lane < 10, pltpu.roll(lower, (128 - 10 * c) % 128, 1), 0.0)
        low, high = from_low[c : c + 1], from_high[c : c + 1]
        tile = jnp.where(sub == 0, low, jnp.where(sub == 1, high, 0.0))
        total += dot_right(jnp.concatenate([body, tile], axis=0), side[c])
        low = 0.75 * low + 0.25 * body[0:1]
        high = 0.75 * high + 0.25 * body[31:32]
        ends += jnp.where(sub == 2 + 2 * c, low, jnp.where(sub == 3 + 2 * c, high, 0.0))
    last = jnp.concatenate([total[24:32], jnp.where(sub < 2, total[32:40], ends)], axis=0)
    ghost_a[...] = total[0:24]
    ghost_a_in[0] = total[0:24]
    ghost_b[...] = last
    ghost_b_in[0] = last
    copies_a = gather(ghost_a, ghost_a_in, plane_peers, 2)
    copies_b = gather(ghost_b, ghost_b_in, line_peers, 3)
    indices[1].wait()

    def tiles(row, offset, source):
        def take(n, out):
            for s in range(SLOTS):
                at = tab[row, offset + n * SLOTS + s]
                out[s] = source[at >> 2, at & 3]

        return take

    def blocks(offset, source):
        def take(n, out):
            out[...] = source[tab[T_GHOST, offset + n * SLOTS]]

        return take

    arrive(planes_copies[0])
    planes_copies += (passed(tiles(T_PLANE, 0, planes_a_in), planes_a_to, planes_a_at, line_peers, 0),)
    arrive(planes_copies[1])
    planes_copies += (passed(tiles(T_PLANE, 32, planes_b_in), planes_b_to, planes_b_at, plane_peers, 1),)

    arrive(copies_a)
    ghost_copies = passed(blocks(0, ghost_a_in), ghost_a_to, ghost_a_at, line_peers, 2)
    arrive(copies_b)
    ghost_copies += passed(blocks(32, ghost_b_in), ghost_b_to, ghost_b_at, plane_peers, 3)
    arrive(planes_copies[2])
    arrive(planes_copies[3])
    arrive(ghost_copies)

    block = jnp.concatenate([ghost_a_at[tab[T_GHOST_AT, 0]], ghost_b_at[tab[T_GHOST_AT, 32]]], axis=0)
    pulled = dot_right(dot_left(along[...], block), spread[...])
    for q in range(SLOTS):
        pull[q] = pulled[q * F : q * F + F]
    faces = dot_right(block[32:40], face[...])

    lane = lax.broadcasted_iota(jnp.int32, (F, F * F), 1)
    row = lax.broadcasted_iota(jnp.int32, (F, F * F), 0)
    for s in range(SLOTS):
        rate = RATE * visc[s]
        ghosts = pull[tab[T_BOX, s]]
        active = tab[T_ACTIVE, s] > 0
        planes = (planes_a_at[tab[T_PLANE_AT, s], s], planes_b_at[tab[T_PLANE_AT, 32 + s], s])
        has_near = (tab[T_NEAR, s] > 0, tab[T_NEAR, 32 + s] > 0)
        for c in range(3):
            cells = fine[c, s]
            ends = [
                jnp.where(
                    has_near[d],
                    jnp.concatenate([planes[d][2 * c : 2 * c + 1], planes[d][2 * c + 1 : 2 * c + 2]], axis=1),
                    faces[2 + 2 * c + d : 3 + 2 * c + d],
                )
                for d in range(2)
            ]
            around = ghosts[:, c * F * F : (c + 1) * F * F] - 6.0 * cells
            around += jnp.where(row == 0, ends[0], pltpu.roll(cells, 1, 0))
            around += jnp.where(row == F - 1, ends[1], pltpu.roll(cells, F - 1, 0))
            around += jnp.where(lane < F, 0.0, pltpu.roll(cells, F, 1))
            around += jnp.where(lane >= F * F - F, 0.0, pltpu.roll(cells, F * F - F, 1))
            around += jnp.where(lane % F == 0, 0.0, pltpu.roll(cells, 1, 1))
            around += jnp.where(lane % F == F - 1, 0.0, pltpu.roll(cells, F * F - 1, 1))
            moved = cells + rate * around
            result[c, s] = jnp.where(active, moved, 0.0)
            adv[(c * SLOTS + s) * F : (c * SLOTS + s + 1) * F, :] = moved

    summed = dot_right(adv[...], pair_yz[...])
    mean = dot_left(pair_x[0], summed[:, 0:128]) + dot_left(pair_x[1], summed[:, 128:256])
    for s in range(SLOTS):
        for part, (out, out_in) in enumerate(((means_a, means_a_in), (means_b, means_b_in))):
            tile = mean[part * 32 + s * 8 : part * 32 + s * 8 + 6]
            out[s] = tile
            out_in[0, s] = tile
    facts = (spots[W_Y, 9], spots[W_Z, 9], tab[T_HERE, 0])
    facts = sum(jnp.where(lane[0:1] == n, v.astype(jnp.float32), 0.0) for n, v in enumerate(facts))
    result[2, SLOTS, 0:1, :] = facts
    copies_a = gather(means_a, means_a_in, plane_peers, 4)
    copies_b = gather(means_b, means_b_in, line_peers, 5)
    arrive(copies_a)
    means_copies = passed(tiles(T_MEAN, 0, means_a_in), means_a_to, means_a_at, line_peers, 4)
    arrive(copies_b)
    means_copies += passed(tiles(T_MEAN, 32, means_b_in), means_b_to, means_b_at, plane_peers, 5)
    arrive(means_copies)
    for q in range(SLOTS):
        spot = (SLOTS, slice(q // 2 * 8, q // 2 * 8 + 6), slice(q % 2 * 128, q % 2 * 128 + 128))
        result[0, *spot] = means_a_at[tab[T_MEAN_AT, q], q]
        result[1, *spot] = means_b_at[tab[T_MEAN_AT, 32 + q], q]
    for copy in started:
        copy.wait_send()


def place_kernel(result, coarse, fine_out, out, column, sems):
    fine_write = pltpu.make_async_copy(result.at[:, 0:SLOTS], fine_out, sems.at[8])
    fine_write.start()
    lane = lax.broadcasted_iota(jnp.int32, (8, 128), 1)
    facts = result[2, SLOTS, 0:1, 0:128]
    y, z, here = (jnp.sum(jnp.where(lane[0:1] == n, facts, 0.0)).astype(jnp.int32) for n in range(3))
    shift = z & 127
    keep = (lane >= shift) & (lane < shift + 8) & (here > 0)
    mine = (y >> 3) * 2 + (z >> 7)
    rest = []
    for n in range(8):
        part = (slice(None), slice(None), pl.ds(n // 2 * 8, 8), pl.ds(n % 2 * 128, 128))
        rest.append(pltpu.make_async_copy(coarse.at[part], out.at[part], sems.at[n]))
    for n in range(8):
        pl.when(mine != n)(rest[n].start)
    y = pl.multiple_of(y, 8)
    z = pl.multiple_of(z - shift, 128)
    writes = []
    for c in range(3):
        for q in range(SLOTS):
            for a in range(B):
                r = 2 * c + a // 2 % 2 + q // 2 * 8
                line = result[a // 4, SLOTS, r : r + 1, q % 2 * 128 : q % 2 * 128 + 128]
                line = jnp.broadcast_to(line, (8, 128))
                line = pltpu.roll(pltpu.roll(line, 72 - 64 * (a % 2), 1, stride=8, stride_axis=0), shift, 1)
                old = coarse[c, q * B + a, pl.ds(y, 8), pl.ds(z, 128)]
                column[c, q * B + a] = jnp.where(keep, line, old)
        spot = out.at[c, :, pl.ds(y, 8), pl.ds(z, 128)]
        writes.append(pltpu.make_async_copy(column.at[c], spot, sems.at[9 + c]))
        writes[-1].start()
    for n in range(8):
        pl.when(mine != n)(rest[n].wait)
    for copy in writes + [fine_write]:
        copy.wait()


def spec(space):
    return pl.BlockSpec(memory_space=space)


def on_device(coarse, fine, visc, corners, grid_slot, neighbors):
    f32 = jnp.float32
    dma = pltpu.SemaphoreType.DMA
    weights = [jnp.asarray(v, jnp.bfloat16) for v in constants()]
    tiles, a, b = (SLOTS, 6, 128), (24, 128), (16, 128)
    sides = (tiles, tiles, a, b, tiles, tiles)
    gathered = [((PLANE, LINE)[n % 2],) + shape for n, shape in enumerate(sides)]
    onward = [((LINE, PLANE)[n % 2],) + shape for n, shape in enumerate(sides)]
    result = pl.pallas_call(
        exchange_kernel,
        out_shape=jax.ShapeDtypeStruct((3, SLOTS + 1, F, F * F), f32),
        in_specs=[spec(pltpu.HBM)] * (6 + len(weights)),
        out_specs=spec(VMEM),
        scratch_shapes=[
            VMEM((3, corners.shape[0]), jnp.int32),
            VMEM((1, corners.shape[0]), jnp.int32),
            VMEM((2, corners.shape[0]), jnp.int32),
            VMEM(fine.shape, f32),
            VMEM(visc.shape, f32),
        ]
        + [VMEM(w.shape, w.dtype) for w in weights]
        + [
            VMEM((T_ROWS, 128), jnp.int32),
            pltpu.SMEM((T_ROWS, 128), jnp.int32),
            VMEM((W_ROWS, 128), jnp.int32),
            pltpu.SMEM((W_ROWS, 128), jnp.int32),
            VMEM((2, 3, 32, PITCH, 128), f32),
            VMEM((3, 32, 128), f32),
            VMEM((3, 32, 128), f32),
            VMEM((4, 32, 128), f32),
            VMEM((3, 32, 128), f32),
            VMEM((4, 32, 128), f32),
            VMEM((12, 8, 128), f32),
            VMEM((12, 8, 128), f32),
            VMEM((SLOTS, F, 3 * F * F), f32),
            VMEM((3 * SLOTS * F, F * F), f32),
        ]
        + [VMEM(shape, f32) for shape in (*sides, *gathered, *onward, *onward)]
        + [dma((5 + len(weights),)), dma((4,)), dma((5,)), dma((5,)), dma((12,)), dma((12,))]
        + [dma((6, PLANE))] * 4,
        compiler_params=pltpu.CompilerParams(collective_id=1, has_side_effects=True),
        name="exchange",
    )(
        corners.T, grid_slot.reshape(1, -1), neighbors.T, coarse, fine, visc,
        *weights,
    )
    return pl.pallas_call(
        place_kernel,
        out_shape=(jax.ShapeDtypeStruct(fine.shape, f32), jax.ShapeDtypeStruct(coarse.shape, f32)),
        in_specs=[spec(VMEM), spec(VMEM)],
        out_specs=(spec(pl.ANY), spec(pl.ANY)),
        scratch_shapes=[VMEM((3, 32, 8, 128), f32), dma((12,))],
        compiler_params=pltpu.CompilerParams(vmem_limit_bytes=16 << 20),
        name="place",
    )(result, coarse)


def solution(mesh):
    split = Mesh(
        mesh.devices.reshape(NXC, NZC, mesh.shape["gy"], mesh.shape["gz"]), ("gx_0", "gx_1", "gy", "gz")
    )
    in_specs = (
        P(None, GX, "gy", "gz"),
        P(None, GX_GY_GZ, None, None),
        P(GX_GY_GZ, None, None),
        P(),
        P(),
        P(),
    )
    out_specs = (P(None, GX_GY_GZ, None, None), P(None, GX, "gy", "gz"))
    return jax.shard_map(on_device, mesh=split, in_specs=in_specs, out_specs=out_specs, check_vma=False)
```

```python
import numpy as np
import jax
import jax.numpy as jnp
from jax import lax
from jax.experimental import pallas as pl
from jax.experimental.pallas import tpu as pltpu
from jax.sharding import Mesh
from jax.sharding import PartitionSpec as P

MESH = pl.DeviceIdType.MESH
VMEM = pltpu.VMEM
GX = ("gx_0", "gx_1")
GX_GY_GZ = ("gx_0", "gx_1", "gy", "gz")
B = 8
F = 16
SLOTS = 4
NXC, NZC, NYC = 4, 8, 4
RATE = 0.15
PITCH = 40

T_PLANE = 0
T_GHOST = 1
T_MEAN = 2
T_PLANE_AT = 3
T_GHOST_AT = 4
T_MEAN_AT = 5
T_NEAR = 6
T_ACTIVE = 7
T_BOX = 8
T_HERE = 9
T_ROWS = 16
W_Y, W_Z = 0, 1
W_ROWS = 8
LINE, PLANE = NZC, NXC * NYC


def interpolation():
    t = np.zeros((F, B + 2), np.float32)
    for i in range(F):
        center = i // 2 + 1
        t[i, center] += 0.75
        t[i, center - 1 if i % 2 == 0 else center + 1] += 0.25
    return t


def constants():
    t = interpolation()
    low = np.zeros(B + 2, np.float32)
    low[0], low[1] = 0.75, 0.25
    high = low[::-1]
    side = np.zeros((3, 128, 128), np.float32)
    for c in range(3):
        for a in range(B + 2):
            for b in range(B + 2):
                side[c, a * 10 + b, c * 40 + b] += low[a]
                side[c, a * 10 + b, c * 40 + 10 + b] += high[a]
                side[c, a * 10 + b, c * 40 + 20 + a] += low[b]
                side[c, a * 10 + b, c * 40 + 30 + a] += high[b]
    along = np.zeros((SLOTS * F, 40), np.float32)
    for q in range(SLOTS):
        for i in range(F):
            for a in range(B + 2):
                x = 8 * q - 1 + a
                along[q * F + i, 32 if x < 0 else 33 if x > 31 else x] += t[i, a]
    spread = np.zeros((128, 3, F, F), np.float32)
    for c in range(3):
        for u in range(B + 2):
            spread[c * 40 + u, c, 0, :] += t[:, u]
            spread[c * 40 + 10 + u, c, F - 1, :] += t[:, u]
            spread[c * 40 + 20 + u, c, :, 0] += t[:, u]
            spread[c * 40 + 30 + u, c, :, F - 1] += t[:, u]
    face = np.zeros((128, F, F), np.float32)
    face[:100] = np.einsum("ja,lb->abjl", t, t).reshape(100, F, F)
    pair_yz = np.zeros((F, F, 256), np.float32)
    for h in range(2):
        for j in range(F):
            for l in range(F):
                pair_yz[j, l, h * 128 + h * 64 + (7 - j // 2) * 8 + l // 2] = 0.25
    pair_x = np.zeros((2, 2, SLOTS, 8, 3, SLOTS, F), np.float32)
    for part in range(2):
        for h in range(2):
            for s in range(SLOTS):
                for c in range(3):
                    for r in range(2):
                        i = 2 * (2 * (2 * part + r) + h)
                        pair_x[h, part, s, 2 * c + r, c, s, i : i + 2] = 0.5
    return (
        side,
        along,
        spread.reshape(128, 3 * F * F),
        face.reshape(128, F * F),
        pair_yz.reshape(F * F, 256),
        pair_x.reshape(2, 2 * SLOTS * 8, 3 * SLOTS * F),
    )


def pick(mask, value):
    return jnp.max(jnp.where(mask, value, -1), axis=1, keepdims=True)


def brick_of(corners):
    return ((corners[0:1] >> 5) * NYC + (corners[1:2] >> 5)) * 2 + (corners[2:3] >> 8)


def as_rows(columns, rows):
    lane = lax.broadcasted_iota(jnp.int32, (1, 128), 1)
    table = jnp.zeros((128, 128), jnp.int32)
    for j, column in enumerate(columns):
        column = jnp.concatenate([column, jnp.zeros((128 - column.shape[0], 1), jnp.int32)], axis=0)
        table = jnp.where(lane == j, column, table)
    return table.T[0:rows]


def window_table(corners, ix, iz, iy, ik):
    place = (corners[1:2] & 31) * 256 + (corners[2:3] & 255)
    n = lax.broadcasted_iota(jnp.int32, (24, 1), 0)
    x = (ix * NZC + iz + (n & 3) - 1) & 31
    y = (iy + (n >> 3) - 1) & 3
    k = (ik + (n >> 2)) & 1
    found = jnp.maximum(pick((x * NYC + y) * 2 + k == brick_of(corners), place), 0)
    return as_rows([(found >> 8) + (y - iy) * 32, (found & 255) + (k - ik) * 256], W_ROWS)


def index_table(corners, grid_slot, near, ix, iz, iy, ik):
    i32 = jnp.int32
    gs = grid_slot[...]
    brick = brick_of(corners)
    box = (corners[0:1] >> 3) & 3
    total = gs.shape[1]
    grids = lax.broadcasted_iota(i32, (1, total), 1)

    def lies(n):
        return n >> 6, (n >> 3) & 7, (n >> 1) & 3

    def turn(x, y):
        return ((ix - x) & 3) * NYC + ((iy - y) & 3)

    def block(count, device, side, gather, at):
        n = lax.broadcasted_iota(i32, (count, 1), 0)
        slot = device(n >> 2) * SLOTS + (n & 3)
        own = gs == slot
        beside = pick(own, near[side : side + 1])
        near_slot = jnp.maximum(pick(grids == beside, gs), 0)
        source = jnp.maximum(pick((gs >> 2) == (slot >> 2), brick), 0)
        home = pick(brick * SLOTS + box == slot, gs)
        held = jnp.maximum(home, 0)
        mine = pick(own, box)
        return (
            gather(near_slot >> 2) * SLOTS + (near_slot & 3),
            gather(source),
            gather(held >> 2) * SLOTS + (held & 3),
            at(near_slot >> 2),
            at(source),
            at(held >> 2),
            (beside >= 0).astype(i32),
            (mine >= 0).astype(i32),
            jnp.maximum(mine, 0),
            (home >= 0).astype(i32),
        )

    def plane_gather(d):
        x, z, y = lies(d)
        return jnp.where(z == iz, turn(x, y), 0)

    def line_gather(d):
        x, z, y = lies(d)
        return jnp.where((x == ix) & (y == iy), (iz - z) & 7, 0)

    def line_at(d):
        return (iz - lies(d)[1]) & 7

    def plane_at(d):
        x, _, y = lies(d)
        return turn(x, y)

    along = block(
        LINE * SLOTS,
        lambda o: ((ix * NZC + ((iz + o) & 7)) * NYC + iy) * 2 + ik,
        0, plane_gather, line_at,
    )
    across = block(
        PLANE * SLOTS,
        lambda o: ((((ix + (o >> 2)) & 3) * NZC + iz) * NYC + ((iy + o) & 3)) * 2 + ik,
        1, line_gather, plane_at,
    )
    return as_rows([jnp.concatenate([a, b], axis=0) for a, b in zip(along, across)], T_ROWS)


class Window:
    def __init__(self, tab, flat, dy, core, dx):
        at = (dy + 1) * 8 + core * 4 + dx + 1
        self.flat, self.y, self.z = flat, tab[W_Y, at], tab[W_Z, at]
        z = self.z & 255
        self.half, shift = z >> 7, z & 127
        self.first = (shift - 1) & 127
        self.lane = lax.broadcasted_iota(jnp.int32, (1, 128), 1)
        self.cross = ((shift == 0) & (self.lane == 127)) | ((shift == 120) & (self.lane == 0))

    def row(self, c, yy, base, x=None):
        y = self.y - 1 + yy
        inside = (y >= 0) & (y < 32)
        y = jnp.clip(y, 0, 31)

        def take(half):
            start = half * (3 * 32 * PITCH) + c * (32 * PITCH) + y
            if x is None:
                return self.flat[pl.ds(start, 32, stride=PITCH), :]
            return self.flat[pl.ds(start + x * PITCH, 1), :]

        line = jnp.where(self.cross, take(1 - self.half), take(self.half))
        line = pltpu.roll(line, (base - self.first) & 127, 1)
        t = self.lane - base
        z = self.z - 1 + t
        keep = (t >= 0) & (t < 10) & (z >= 0) & (z < 256) & inside
        return jnp.where(keep, line, 0.0)


def parts_of(a):
    first = a.astype(jnp.bfloat16)
    a = a - first.astype(jnp.float32)
    second = a.astype(jnp.bfloat16)
    return first, second, (a - second.astype(jnp.float32)).astype(jnp.bfloat16)


def dot_right(a, weights):
    return sum(jnp.dot(p, weights, preferred_element_type=jnp.float32) for p in parts_of(a))


def dot_left(weights, a):
    return sum(jnp.dot(weights, p, preferred_element_type=jnp.float32) for p in parts_of(a))


def exchange_kernel(
    corners_in, grid_slot_in, near_in, coarse, fine_in, visc_in, side_in, along_in, spread_in, face_in,
    pair_yz_in, pair_x_in,
    result,
    corners, grid_slot, near, fine, visc, side, along, spread, face, pair_yz, pair_x,
    table, tab, places, spots, brick, own, other, beside, near_z, near_y, edge, edges, pull, adv,
    planes_a, planes_b, ghost_a, ghost_b, means_a, means_b,
    planes_a_in, planes_b_in, ghost_a_in, ghost_b_in, means_a_in, means_b_in,
    planes_a_to, planes_b_to, ghost_a_to, ghost_b_to, means_a_to, means_b_to,
    planes_a_at, planes_b_at, ghost_a_at, ghost_b_at, means_a_at, means_b_at,
    input_sems, local, y_send, y_recv, x_send, x_recv, gather_send, gather_recv, pass_send, pass_recv,
):
    ix, iz = lax.axis_index("gx_0"), lax.axis_index("gx_1")
    iy, ik = lax.axis_index("gy"), lax.axis_index("gz")

    def device(x, z, y, k):
        return {"gx_0": x, "gx_1": z, "gy": y, "gz": k}

    def far(n, count):
        return min(n, count - n)

    plane_peers = [
        (n, device(lax.rem(ix + n // NYC, NXC), iz, lax.rem(iy + n % NYC, NYC), ik))
        for n in sorted(range(1, PLANE), key=lambda n: -far(n // NYC, NXC) - far(n % NYC, NYC))
    ]
    line_peers = [
        (n, device(ix, lax.rem(iz + n, NZC), iy, ik)) for n in sorted(range(1, LINE), key=lambda n: -far(n, NZC))
    ]
    chain = ix * NZC + iz
    beside_of = ((-1, 0), (-1, 1), (1, 0), (1, 1))
    y_peers = [
        (n, device(ix, iz, lax.rem(iy + NYC + dy, NYC), lax.rem(ik + dk, 2))) for n, (dy, dk) in enumerate(beside_of)
    ]
    partner = device(ix, iz, iy, 1 - ik)
    around_of = [(dy, core) for dy in (-1, 1, 0) for core in (0, 1)]
    edge_peers = []
    for side_x, step in enumerate((1, 31)):
        x = lax.rem(chain + step, 32)
        for n, (dy, core) in enumerate(around_of):
            edge_peers.append(
                (side_x * 6 + n, device(lax.div(x, NZC), lax.rem(x, NZC), lax.rem(iy + NYC + dy, NYC), lax.rem(ik + core, 2)))
            )
    started = []

    def send(src, dst, send_sem, recv_sem, to):
        copy = pltpu.make_async_remote_copy(
            src_ref=src, dst_ref=dst, send_sem=send_sem, recv_sem=recv_sem, device_id=to, device_id_type=MESH
        )
        copy.start()
        started.append(copy)
        return copy

    def gather(src, dst, peers, item):
        return [
            send(src, dst.at[n], gather_send.at[item, n], gather_recv.at[item, n], to) for n, to in peers
        ]

    def passed(take, to_ref, at_ref, peers, item):
        copies = []
        for n, to in peers:
            take(n, to_ref.at[n])
            copies.append(send(to_ref.at[n], at_ref.at[n], pass_send.at[item, n], pass_recv.at[item, n], to))
        take(0, at_ref.at[0])
        return copies

    def arrive(copies):
        for copy in copies:
            copy.wait_recv()

    loads = [
        pltpu.make_async_copy(
            coarse.at[:, :, :, pl.ds(h * 128, 128)], brick.at[h, :, :, pl.ds(0, 32), :], local.at[h]
        )
        for h in range(2)
    ]
    inputs = [
        pltpu.make_async_copy(src, dst, input_sems.at[n])
        for n, (src, dst) in enumerate(
            (
                (corners_in, corners), (grid_slot_in, grid_slot), (near_in, near), (fine_in, fine),
                (visc_in, visc), (side_in, side), (along_in, along), (spread_in, spread),
                (face_in, face), (pair_yz_in, pair_yz), (pair_x_in, pair_x),
            )
        )
    ]
    for copy in inputs[:4] + loads + inputs[4:]:
        copy.start()
    barrier = pltpu.get_barrier_semaphore()
    greeted = plane_peers + line_peers + edge_peers + [y_peers[1], y_peers[3], (0, partner)]
    for _, to in greeted:
        pl.semaphore_signal(barrier, inc=1, device_id=to, device_id_type=MESH)

    inputs[0].wait()
    places[...] = window_table(corners, ix, iz, iy, ik)
    indices = [pltpu.make_async_copy(places, spots, local.at[2]), pltpu.make_async_copy(table, tab, local.at[3])]
    indices[0].start()

    inputs[3].wait()
    for s in range(SLOTS):
        for x, out, out_in in ((F - 1, planes_a, planes_a_in), (0, planes_b, planes_b_in)):
            rows = [fine[c, s, x : x + 1, h * 128 : h * 128 + 128] for c in range(3) for h in range(2)]
            tile = jnp.concatenate(rows, axis=0)
            out[s] = tile
            out_in[0, s] = tile
    pl.semaphore_wait(barrier, len(greeted))

    indices[0].wait()
    for copy in loads + inputs[4:]:
        copy.wait()
    flat = brick.reshape(2 * 3 * 32 * PITCH, 128)
    lane = lax.broadcasted_iota(jnp.int32, (1, 128), 1)
    sub = lax.broadcasted_iota(jnp.int32, (8, 128), 0)

    def cut(dy, core, rows, out):
        mid = Window(spots, flat, dy, core, 0)
        out[...] = sum(mid.row(c, yy, base) for c, yy, base in rows)

    def cut_edges(n, dy, core):
        for side_x, x in enumerate((31, 0)):
            window = Window(spots, flat, dy, core, 1 - 2 * side_x)
            tile = jnp.zeros((8, 128), jnp.float32)
            for c in range(3):
                lines = [(9,), (0,), range(10)][(-1, 1, 0).index(dy)]
                line = sum(window.row(c, yy, yy * 10, x) for yy in lines)
                tile = jnp.where(sub == c, line, tile)
            edge[side_x * 6 + n] = tile

    first = []
    for n, to in y_peers:
        dy, core = beside_of[n]
        cut(dy, core, [(c, 9 if dy < 0 else 0, c * 10) for c in range(3)], beside.at[n])
        first.append(send(beside.at[n], near_y.at[n], y_send.at[n], y_recv.at[n], to))
    for n, (dy, core) in enumerate(around_of):
        cut_edges(n, dy, core)
        for at in (n, 6 + n):
            first.append(send(edge.at[at], edges.at[at], x_send.at[at], x_recv.at[at], edge_peers[at][1]))
    for core, out in ((1, other), (0, own)):
        for c in range(3):
            cut(0, core, [(c, yy, yy * 10) for yy in range(10)], out.at[c])
        if core:
            first.append(send(other, near_z, y_send.at[4], y_recv.at[4], partner))
    planes_copies = (
        gather(planes_a, planes_a_in, plane_peers, 0),
        gather(planes_b, planes_b_in, line_peers, 1),
    )
    for copy in inputs[1:3]:
        copy.wait()
    table[...] = index_table(corners, grid_slot, near, ix, iz, iy, ik)
    indices[1].start()
    arrive(first)
    upper = near_y[0] + near_y[1]
    lower = near_y[2] + near_y[3]
    from_low = jnp.where(chain > 0, sum(edges[n] for n in range(6)), 0.0)
    from_high = jnp.where(chain < 31, sum(edges[n] for n in range(6, 12)), 0.0)
    total = jnp.zeros((40, 128), jnp.float32)
    ends = jnp.zeros((8, 128), jnp.float32)
    for c in range(3):
        body = own[c] + near_z[c]
        body += jnp.where((lane >= 90) & (lane < 100), pltpu.roll(upper, 90 - 10 * c, 1), 0.0)
        body += jnp.where(lane < 10, pltpu.roll(lower, (128 - 10 * c) % 128, 1), 0.0)
        low, high = from_low[c : c + 1], from_high[c : c + 1]
        tile = jnp.where(sub == 0, low, jnp.where(sub == 1, high, 0.0))
        total += dot_right(jnp.concatenate([body, tile], axis=0), side[c])
        low = 0.75 * low + 0.25 * body[0:1]
        high = 0.75 * high + 0.25 * body[31:32]
        ends += jnp.where(sub == 2 + 2 * c, low, jnp.where(sub == 3 + 2 * c, high, 0.0))
    last = jnp.concatenate([total[24:32], jnp.where(sub < 2, total[32:40], ends)], axis=0)
    ghost_a[...] = total[0:24]
    ghost_a_in[0] = total[0:24]
    ghost_b[...] = last
    ghost_b_in[0] = last
    copies_a = gather(ghost_a, ghost_a_in, plane_peers, 2)
    copies_b = gather(ghost_b, ghost_b_in, line_peers, 3)
    indices[1].wait()

    def tiles(row, offset, source):
        def take(n, out):
            for s in range(SLOTS):
                at = tab[row, offset + n * SLOTS + s]
                out[s] = source[at >> 2, at & 3]

        return take

    def blocks(offset, source):
        def take(n, out):
            out[...] = source[tab[T_GHOST, offset + n * SLOTS]]

        return take

    arrive(planes_copies[0])
    planes_copies += (passed(tiles(T_PLANE, 0, planes_a_in), planes_a_to, planes_a_at, line_peers, 0),)
    arrive(planes_copies[1])
    planes_copies += (passed(tiles(T_PLANE, 32, planes_b_in), planes_b_to, planes_b_at, plane_peers, 1),)

    arrive(copies_a)
    ghost_copies = passed(blocks(0, ghost_a_in), ghost_a_to, ghost_a_at, line_peers, 2)
    arrive(copies_b)
    ghost_copies += passed(blocks(32, ghost_b_in), ghost_b_to, ghost_b_at, plane_peers, 3)
    arrive(planes_copies[2])
    arrive(planes_copies[3])
    arrive(ghost_copies)

    block = jnp.concatenate([ghost_a_at[tab[T_GHOST_AT, 0]], ghost_b_at[tab[T_GHOST_AT, 32]]], axis=0)
    pulled = dot_right(dot_left(along[...], block), spread[...])
    for q in range(SLOTS):
        pull[q] = pulled[q * F : q * F + F]
    faces = dot_right(block[32:40], face[...])

    lane = lax.broadcasted_iota(jnp.int32, (F, F * F), 1)
    row = lax.broadcasted_iota(jnp.int32, (F, F * F), 0)
    for s in range(SLOTS):
        rate = RATE * visc[s]
        ghosts = pull[tab[T_BOX, s]]
        active = tab[T_ACTIVE, s] > 0
        planes = (planes_a_at[tab[T_PLANE_AT, s], s], planes_b_at[tab[T_PLANE_AT, 32 + s], s])
        has_near = (tab[T_NEAR, s] > 0, tab[T_NEAR, 32 + s] > 0)
        for c in range(3):
            cells = fine[c, s]
            ends = [
                jnp.where(
                    has_near[d],
                    jnp.concatenate([planes[d][2 * c : 2 * c + 1], planes[d][2 * c + 1 : 2 * c + 2]], axis=1),
                    faces[2 + 2 * c + d : 3 + 2 * c + d],
                )
                for d in range(2)
            ]
            around = ghosts[:, c * F * F : (c + 1) * F * F] - 6.0 * cells
            around += jnp.where(row == 0, ends[0], pltpu.roll(cells, 1, 0))
            around += jnp.where(row == F - 1, ends[1], pltpu.roll(cells, F - 1, 0))
            around += jnp.where(lane < F, 0.0, pltpu.roll(cells, F, 1))
            around += jnp.where(lane >= F * F - F, 0.0, pltpu.roll(cells, F * F - F, 1))
            around += jnp.where(lane % F == 0, 0.0, pltpu.roll(cells, 1, 1))
            around += jnp.where(lane % F == F - 1, 0.0, pltpu.roll(cells, F * F - 1, 1))
            moved = cells + rate * around
            result[c, s] = jnp.where(active, moved, 0.0)
            adv[(c * SLOTS + s) * F : (c * SLOTS + s + 1) * F, :] = moved

    summed = dot_right(adv[...], pair_yz[...])
    mean = dot_left(pair_x[0], summed[:, 0:128]) + dot_left(pair_x[1], summed[:, 128:256])
    for s in range(SLOTS):
        for part, (out, out_in) in enumerate(((means_a, means_a_in), (means_b, means_b_in))):
            tile = mean[part * 32 + s * 8 : part * 32 + s * 8 + 6]
            out[s] = tile
            out_in[0, s] = tile
    facts = (spots[W_Y, 9], spots[W_Z, 9], tab[T_HERE, 0])
    facts = sum(jnp.where(lane[0:1] == n, v.astype(jnp.float32), 0.0) for n, v in enumerate(facts))
    result[2, SLOTS, 0:1, :] = facts
    copies_a = gather(means_a, means_a_in, plane_peers, 4)
    copies_b = gather(means_b, means_b_in, line_peers, 5)
    arrive(copies_a)
    means_copies = passed(tiles(T_MEAN, 0, means_a_in), means_a_to, means_a_at, line_peers, 4)
    arrive(copies_b)
    means_copies += passed(tiles(T_MEAN, 32, means_b_in), means_b_to, means_b_at, plane_peers, 5)
    arrive(means_copies)
    for q in range(SLOTS):
        spot = (SLOTS, slice(q // 2 * 8, q // 2 * 8 + 6), slice(q % 2 * 128, q % 2 * 128 + 128))
        result[0, *spot] = means_a_at[tab[T_MEAN_AT, q], q]
        result[1, *spot] = means_b_at[tab[T_MEAN_AT, 32 + q], q]
    for copy in started:
        copy.wait_send()


def place_kernel(result, coarse, fine_out, out, column, sems):
    fine_write = pltpu.make_async_copy(result.at[:, 0:SLOTS], fine_out, sems.at[8])
    fine_write.start()
    lane = lax.broadcasted_iota(jnp.int32, (8, 128), 1)
    facts = result[2, SLOTS, 0:1, 0:128]
    y, z, here = (jnp.sum(jnp.where(lane[0:1] == n, facts, 0.0)).astype(jnp.int32) for n in range(3))
    shift = z & 127
    keep = (lane >= shift) & (lane < shift + 8) & (here > 0)
    mine = (y >> 3) * 2 + (z >> 7)
    rest = []
    for n in range(8):
        part = (slice(None), slice(None), pl.ds(n // 2 * 8, 8), pl.ds(n % 2 * 128, 128))
        rest.append(pltpu.make_async_copy(coarse.at[part], out.at[part], sems.at[n]))
    for n in range(8):
        pl.when(mine != n)(rest[n].start)
    y = pl.multiple_of(y, 8)
    z = pl.multiple_of(z - shift, 128)
    writes = []
    for c in range(3):
        for q in range(SLOTS):
            for a in range(B):
                r = 2 * c + a // 2 % 2 + q // 2 * 8
                line = result[a // 4, SLOTS, r : r + 1, q % 2 * 128 : q % 2 * 128 + 128]
                line = jnp.broadcast_to(line, (8, 128))
                line = pltpu.roll(pltpu.roll(line, 72 - 64 * (a % 2), 1, stride=8, stride_axis=0), shift, 1)
                old = coarse[c, q * B + a, pl.ds(y, 8), pl.ds(z, 128)]
                column[c, q * B + a] = jnp.where(keep, line, old)
        spot = out.at[c, :, pl.ds(y, 8), pl.ds(z, 128)]
        writes.append(pltpu.make_async_copy(column.at[c], spot, sems.at[9 + c]))
        writes[-1].start()
    for n in range(8):
        pl.when(mine != n)(rest[n].wait)
    for copy in writes + [fine_write]:
        copy.wait()


def spec(space):
    return pl.BlockSpec(memory_space=space)


def on_device(coarse, fine, visc, corners, grid_slot, neighbors):
    f32 = jnp.float32
    dma = pltpu.SemaphoreType.DMA
    weights = [jnp.asarray(v, jnp.bfloat16) for v in constants()]
    tiles, a, b = (SLOTS, 6, 128), (24, 128), (16, 128)
    sides = (tiles, tiles, a, b, tiles, tiles)
    gathered = [((PLANE, LINE)[n % 2],) + shape for n, shape in enumerate(sides)]
    onward = [((LINE, PLANE)[n % 2],) + shape for n, shape in enumerate(sides)]
    result = pl.pallas_call(
        exchange_kernel,
        out_shape=jax.ShapeDtypeStruct((3, SLOTS + 1, F, F * F), f32),
        in_specs=[spec(pltpu.HBM)] * (6 + len(weights)),
        out_specs=spec(VMEM),
        scratch_shapes=[
            VMEM((3, corners.shape[0]), jnp.int32),
            VMEM((1, corners.shape[0]), jnp.int32),
            VMEM((2, corners.shape[0]), jnp.int32),
            VMEM(fine.shape, f32),
            VMEM(visc.shape, f32),
        ]
        + [VMEM(w.shape, w.dtype) for w in weights]
        + [
            VMEM((T_ROWS, 128), jnp.int32),
            pltpu.SMEM((T_ROWS, 128), jnp.int32),
            VMEM((W_ROWS, 128), jnp.int32),
            pltpu.SMEM((W_ROWS, 128), jnp.int32),
            VMEM((2, 3, 32, PITCH, 128), f32),
            VMEM((3, 32, 128), f32),
            VMEM((3, 32, 128), f32),
            VMEM((4, 32, 128), f32),
            VMEM((3, 32, 128), f32),
            VMEM((4, 32, 128), f32),
            VMEM((12, 8, 128), f32),
            VMEM((12, 8, 128), f32),
            VMEM((SLOTS, F, 3 * F * F), f32),
            VMEM((3 * SLOTS * F, F * F), f32),
        ]
        + [VMEM(shape, f32) for shape in (*sides, *gathered, *onward, *onward)]
        + [dma((5 + len(weights),)), dma((4,)), dma((5,)), dma((5,)), dma((12,)), dma((12,))]
        + [dma((6, PLANE))] * 4,
        compiler_params=pltpu.CompilerParams(collective_id=1, has_side_effects=True),
        name="exchange",
    )(
        corners.T, grid_slot.reshape(1, -1), neighbors.T, coarse, fine, visc,
        *weights,
    )
    return pl.pallas_call(
        place_kernel,
        out_shape=(jax.ShapeDtypeStruct(fine.shape, f32), jax.ShapeDtypeStruct(coarse.shape, f32)),
        in_specs=[spec(VMEM), spec(VMEM)],
        out_specs=(spec(pl.ANY), spec(pl.ANY)),
        scratch_shapes=[VMEM((3, 32, 8, 128), f32), dma((12,))],
        compiler_params=pltpu.CompilerParams(vmem_limit_bytes=16 << 20),
        name="place",
    )(result, coarse)


def solution(mesh):
    split = Mesh(
        mesh.devices.reshape(NXC, NZC, mesh.shape["gy"], mesh.shape["gz"]), ("gx_0", "gx_1", "gy", "gz")
    )
    in_specs = (
        P(None, GX, "gy", "gz"),
        P(None, GX_GY_GZ, None, None),
        P(GX_GY_GZ, None, None),
        P(),
        P(),
        P(),
    )
    out_specs = (P(None, GX_GY_GZ, None, None), P(None, GX, "gy", "gz"))
    return jax.shard_map(on_device, mesh=split, in_specs=in_specs, out_specs=out_specs, check_vma=False)
```

```python
import numpy as np
import jax
import jax.numpy as jnp
from jax import lax
from jax.experimental import pallas as pl
from jax.experimental.pallas import tpu as pltpu
from jax.sharding import Mesh
from jax.sharding import PartitionSpec as P

MESH = pl.DeviceIdType.MESH
VMEM = pltpu.VMEM
GX = ("gx_0", "gx_1")
GX_GY_GZ = ("gx_0", "gx_1", "gy", "gz")
B = 8
F = 16
SLOTS = 4
NXC, NZC, NYC = 4, 8, 4
RATE = 0.15
PITCH = 40

T_PLANE = 0
T_GHOST = 1
T_MEAN = 2
T_PLANE_AT = 3
T_GHOST_AT = 4
T_MEAN_AT = 5
T_NEAR = 6
T_ACTIVE = 7
T_BOX = 8
T_HERE = 9
T_ROWS = 16
W_Y, W_Z = 0, 1
W_ROWS = 8
LINE, PLANE = NZC, NXC * NYC


def interpolation():
    t = np.zeros((F, B + 2), np.float32)
    for i in range(F):
        center = i // 2 + 1
        t[i, center] += 0.75
        t[i, center - 1 if i % 2 == 0 else center + 1] += 0.25
    return t


def constants():
    t = interpolation()
    low = np.zeros(B + 2, np.float32)
    low[0], low[1] = 0.75, 0.25
    high = low[::-1]
    side = np.zeros((3, 128, 128), np.float32)
    for c in range(3):
        for a in range(B + 2):
            for b in range(B + 2):
                side[c, a * 10 + b, c * 40 + b] += low[a]
                side[c, a * 10 + b, c * 40 + 10 + b] += high[a]
                side[c, a * 10 + b, c * 40 + 20 + a] += low[b]
                side[c, a * 10 + b, c * 40 + 30 + a] += high[b]
    along = np.zeros((SLOTS * F, 40), np.float32)
    for q in range(SLOTS):
        for i in range(F):
            for a in range(B + 2):
                x = 8 * q - 1 + a
                along[q * F + i, 32 if x < 0 else 33 if x > 31 else x] += t[i, a]
    spread = np.zeros((128, 3, F, F), np.float32)
    for c in range(3):
        for u in range(B + 2):
            spread[c * 40 + u, c, 0, :] += t[:, u]
            spread[c * 40 + 10 + u, c, F - 1, :] += t[:, u]
            spread[c * 40 + 20 + u, c, :, 0] += t[:, u]
            spread[c * 40 + 30 + u, c, :, F - 1] += t[:, u]
    face = np.zeros((128, F, F), np.float32)
    face[:100] = np.einsum("ja,lb->abjl", t, t).reshape(100, F, F)
    pair_yz = np.zeros((F, F, 256), np.float32)
    for h in range(2):
        for j in range(F):
            for l in range(F):
                pair_yz[j, l, h * 128 + h * 64 + (7 - j // 2) * 8 + l // 2] = 0.25
    pair_x = np.zeros((2, 2, SLOTS, 8, 3, SLOTS, F), np.float32)
    for part in range(2):
        for h in range(2):
            for s in range(SLOTS):
                for c in range(3):
                    for r in range(2):
                        i = 2 * (2 * (2 * part + r) + h)
                        pair_x[h, part, s, 2 * c + r, c, s, i : i + 2] = 0.5
    return (
        side,
        along,
        spread.reshape(128, 3 * F * F),
        face.reshape(128, F * F),
        pair_yz.reshape(F * F, 256),
        pair_x.reshape(2, 2 * SLOTS * 8, 3 * SLOTS * F),
    )


def pick(mask, value):
    return jnp.max(jnp.where(mask, value, -1), axis=1, keepdims=True)


def brick_of(corners):
    return ((corners[0:1] >> 5) * NYC + (corners[1:2] >> 5)) * 2 + (corners[2:3] >> 8)


def as_rows(columns, rows):
    lane = lax.broadcasted_iota(jnp.int32, (1, 128), 1)
    table = jnp.zeros((128, 128), jnp.int32)
    for j, column in enumerate(columns):
        column = jnp.concatenate([column, jnp.zeros((128 - column.shape[0], 1), jnp.int32)], axis=0)
        table = jnp.where(lane == j, column, table)
    return table.T[0:rows]


def window_table(corners, ix, iz, iy, ik):
    place = (corners[1:2] & 31) * 256 + (corners[2:3] & 255)
    n = lax.broadcasted_iota(jnp.int32, (24, 1), 0)
    x = (ix * NZC + iz + (n & 3) - 1) & 31
    y = (iy + (n >> 3) - 1) & 3
    k = (ik + (n >> 2)) & 1
    found = jnp.maximum(pick((x * NYC + y) * 2 + k == brick_of(corners), place), 0)
    return as_rows([(found >> 8) + (y - iy) * 32, (found & 255) + (k - ik) * 256], W_ROWS)


def index_table(corners, grid_slot, near, ix, iz, iy, ik):
    i32 = jnp.int32
    gs = grid_slot[...]
    brick = brick_of(corners)
    box = (corners[0:1] >> 3) & 3
    total = gs.shape[1]
    grids = lax.broadcasted_iota(i32, (1, total), 1)

    def lies(n):
        return n >> 6, (n >> 3) & 7, (n >> 1) & 3

    def turn(x, y):
        return ((ix - x) & 3) * NYC + ((iy - y) & 3)

    def block(count, device, side, gather, at):
        n = lax.broadcasted_iota(i32, (count, 1), 0)
        slot = device(n >> 2) * SLOTS + (n & 3)
        own = gs == slot
        beside = pick(own, near[side : side + 1])
        near_slot = jnp.maximum(pick(grids == beside, gs), 0)
        source = jnp.maximum(pick((gs >> 2) == (slot >> 2), brick), 0)
        home = pick(brick * SLOTS + box == slot, gs)
        held = jnp.maximum(home, 0)
        mine = pick(own, box)
        return (
            gather(near_slot >> 2) * SLOTS + (near_slot & 3),
            gather(source),
            gather(held >> 2) * SLOTS + (held & 3),
            at(near_slot >> 2),
            at(source),
            at(held >> 2),
            (beside >= 0).astype(i32),
            (mine >= 0).astype(i32),
            jnp.maximum(mine, 0),
            (home >= 0).astype(i32),
        )

    def plane_gather(d):
        x, z, y = lies(d)
        return jnp.where(z == iz, turn(x, y), 0)

    def line_gather(d):
        x, z, y = lies(d)
        return jnp.where((x == ix) & (y == iy), (iz - z) & 7, 0)

    def line_at(d):
        return (iz - lies(d)[1]) & 7

    def plane_at(d):
        x, _, y = lies(d)
        return turn(x, y)

    along = block(
        LINE * SLOTS,
        lambda o: ((ix * NZC + ((iz + o) & 7)) * NYC + iy) * 2 + ik,
        0, plane_gather, line_at,
    )
    across = block(
        PLANE * SLOTS,
        lambda o: ((((ix + (o >> 2)) & 3) * NZC + iz) * NYC + ((iy + o) & 3)) * 2 + ik,
        1, line_gather, plane_at,
    )
    return as_rows([jnp.concatenate([a, b], axis=0) for a, b in zip(along, across)], T_ROWS)


class Window:
    def __init__(self, tab, flat, dy, core, dx):
        at = (dy + 1) * 8 + core * 4 + dx + 1
        self.flat, self.y, self.z = flat, tab[W_Y, at], tab[W_Z, at]
        z = self.z & 255
        self.half, shift = z >> 7, z & 127
        self.first = (shift - 1) & 127
        self.lane = lax.broadcasted_iota(jnp.int32, (1, 128), 1)
        self.cross = ((shift == 0) & (self.lane == 127)) | ((shift == 120) & (self.lane == 0))

    def row(self, c, yy, base, x=None):
        y = self.y - 1 + yy
        inside = (y >= 0) & (y < 32)
        y = jnp.clip(y, 0, 31)

        def take(half):
            start = half * (3 * 32 * PITCH) + c * (32 * PITCH) + y
            if x is None:
                return self.flat[pl.ds(start, 32, stride=PITCH), :]
            return self.flat[pl.ds(start + x * PITCH, 1), :]

        line = jnp.where(self.cross, take(1 - self.half), take(self.half))
        line = pltpu.roll(line, (base - self.first) & 127, 1)
        t = self.lane - base
        z = self.z - 1 + t
        keep = (t >= 0) & (t < 10) & (z >= 0) & (z < 256) & inside
        return jnp.where(keep, line, 0.0)


def parts_of(a):
    first = a.astype(jnp.bfloat16)
    a = a - first.astype(jnp.float32)
    second = a.astype(jnp.bfloat16)
    return first, second, (a - second.astype(jnp.float32)).astype(jnp.bfloat16)


def dot_right(a, weights):
    return sum(jnp.dot(p, weights, preferred_element_type=jnp.float32) for p in parts_of(a))


def dot_left(weights, a):
    return sum(jnp.dot(weights, p, preferred_element_type=jnp.float32) for p in parts_of(a))


def exchange_kernel(
    corners_in, grid_slot_in, near_in, coarse, fine_in, visc_in, side_in, along_in, spread_in, face_in,
    pair_yz_in, pair_x_in,
    result,
    corners, grid_slot, near, fine, visc, side, along, spread, face, pair_yz, pair_x,
    table, tab, places, spots, brick, own, other, beside, near_z, near_y, edge, edges, pull, adv,
    planes_a, planes_b, ghost_a, ghost_b, means_a, means_b,
    planes_a_in, planes_b_in, ghost_a_in, ghost_b_in, means_a_in, means_b_in,
    planes_a_to, planes_b_to, ghost_a_to, ghost_b_to, means_a_to, means_b_to,
    planes_a_at, planes_b_at, ghost_a_at, ghost_b_at, means_a_at, means_b_at,
    input_sems, local, y_send, y_recv, x_send, x_recv, gather_send, gather_recv, pass_send, pass_recv,
):
    ix, iz = lax.axis_index("gx_0"), lax.axis_index("gx_1")
    iy, ik = lax.axis_index("gy"), lax.axis_index("gz")

    def device(x, z, y, k):
        return {"gx_0": x, "gx_1": z, "gy": y, "gz": k}

    def far(n, count):
        return min(n, count - n)

    plane_peers = [
        (n, device(lax.rem(ix + n // NYC, NXC), iz, lax.rem(iy + n % NYC, NYC), ik))
        for n in sorted(range(1, PLANE), key=lambda n: -far(n // NYC, NXC) - far(n % NYC, NYC))
    ]
    line_peers = [
        (n, device(ix, lax.rem(iz + n, NZC), iy, ik)) for n in sorted(range(1, LINE), key=lambda n: -far(n, NZC))
    ]
    chain = ix * NZC + iz
    beside_of = ((-1, 0), (-1, 1), (1, 0), (1, 1))
    y_peers = [
        (n, device(ix, iz, lax.rem(iy + NYC + dy, NYC), lax.rem(ik + dk, 2))) for n, (dy, dk) in enumerate(beside_of)
    ]
    partner = device(ix, iz, iy, 1 - ik)
    around_of = [(dy, core) for dy in (-1, 1, 0) for core in (0, 1)]
    edge_peers = []
    for side_x, step in enumerate((1, 31)):
        x = lax.rem(chain + step, 32)
        for n, (dy, core) in enumerate(around_of):
            edge_peers.append(
                (side_x * 6 + n, device(lax.div(x, NZC), lax.rem(x, NZC), lax.rem(iy + NYC + dy, NYC), lax.rem(ik + core, 2)))
            )
    started = []

    def send(src, dst, send_sem, recv_sem, to):
        copy = pltpu.make_async_remote_copy(
            src_ref=src, dst_ref=dst, send_sem=send_sem, recv_sem=recv_sem, device_id=to, device_id_type=MESH
        )
        copy.start()
        started.append(copy)
        return copy

    def gather(src, dst, peers, item):
        return [
            send(src, dst.at[n], gather_send.at[item, n], gather_recv.at[item, n], to) for n, to in peers
        ]

    def passed(take, to_ref, at_ref, peers, item):
        copies = []
        for n, to in peers:
            take(n, to_ref.at[n])
            copies.append(send(to_ref.at[n], at_ref.at[n], pass_send.at[item, n], pass_recv.at[item, n], to))
        take(0, at_ref.at[0])
        return copies

    def arrive(copies):
        for copy in copies:
            copy.wait_recv()

    loads = [
        pltpu.make_async_copy(
            coarse.at[:, :, :, pl.ds(h * 128, 128)], brick.at[h, :, :, pl.ds(0, 32), :], local.at[h]
        )
        for h in range(2)
    ]
    inputs = [
        pltpu.make_async_copy(src, dst, input_sems.at[n])
        for n, (src, dst) in enumerate(
            (
                (corners_in, corners), (grid_slot_in, grid_slot), (near_in, near), (fine_in, fine),
                (visc_in, visc), (side_in, side), (along_in, along), (spread_in, spread),
                (face_in, face), (pair_yz_in, pair_yz), (pair_x_in, pair_x),
            )
        )
    ]
    inputs[0].start()
    barrier = pltpu.get_barrier_semaphore()
    greeted = plane_peers + line_peers + edge_peers + [y_peers[1], y_peers[3], (0, partner)]
    for _, to in greeted:
        pl.semaphore_signal(barrier, inc=1, device_id=to, device_id_type=MESH)
    for copy in inputs[1:4] + loads + inputs[4:]:
        copy.start()

    inputs[0].wait()
    places[...] = window_table(corners, ix, iz, iy, ik)
    indices = [pltpu.make_async_copy(places, spots, local.at[2]), pltpu.make_async_copy(table, tab, local.at[3])]
    indices[0].start()

    inputs[3].wait()
    for s in range(SLOTS):
        for x, out, out_in in ((F - 1, planes_a, planes_a_in), (0, planes_b, planes_b_in)):
            rows = [fine[c, s, x : x + 1, h * 128 : h * 128 + 128] for c in range(3) for h in range(2)]
            tile = jnp.concatenate(rows, axis=0)
            out[s] = tile
            out_in[0, s] = tile
    pl.semaphore_wait(barrier, len(greeted))

    indices[0].wait()
    for copy in loads + inputs[4:]:
        copy.wait()
    flat = brick.reshape(2 * 3 * 32 * PITCH, 128)
    lane = lax.broadcasted_iota(jnp.int32, (1, 128), 1)
    sub = lax.broadcasted_iota(jnp.int32, (8, 128), 0)

    def cut(dy, core, rows, out):
        mid = Window(spots, flat, dy, core, 0)
        out[...] = sum(mid.row(c, yy, base) for c, yy, base in rows)

    def cut_edges(n, dy, core):
        for side_x, x in enumerate((31, 0)):
            window = Window(spots, flat, dy, core, 1 - 2 * side_x)
            tile = jnp.zeros((8, 128), jnp.float32)
            for c in range(3):
                lines = [(9,), (0,), range(10)][(-1, 1, 0).index(dy)]
                line = sum(window.row(c, yy, yy * 10, x) for yy in lines)
                tile = jnp.where(sub == c, line, tile)
            edge[side_x * 6 + n] = tile

    first = []
    for n, to in y_peers:
        dy, core = beside_of[n]
        cut(dy, core, [(c, 9 if dy < 0 else 0, c * 10) for c in range(3)], beside.at[n])
        first.append(send(beside.at[n], near_y.at[n], y_send.at[n], y_recv.at[n], to))
    for n, (dy, core) in enumerate(around_of):
        cut_edges(n, dy, core)
        for at in (n, 6 + n):
            first.append(send(edge.at[at], edges.at[at], x_send.at[at], x_recv.at[at], edge_peers[at][1]))
    for core, out in ((1, other), (0, own)):
        for c in range(3):
            cut(0, core, [(c, yy, yy * 10) for yy in range(10)], out.at[c])
        if core:
            first.append(send(other, near_z, y_send.at[4], y_recv.at[4], partner))
    planes_copies = (
        gather(planes_a, planes_a_in, plane_peers, 0),
        gather(planes_b, planes_b_in, line_peers, 1),
    )
    for copy in inputs[1:3]:
        copy.wait()
    table[...] = index_table(corners, grid_slot, near, ix, iz, iy, ik)
    indices[1].start()
    arrive(first)
    upper = near_y[0] + near_y[1]
    lower = near_y[2] + near_y[3]
    from_low = jnp.where(chain > 0, sum(edges[n] for n in range(6)), 0.0)
    from_high = jnp.where(chain < 31, sum(edges[n] for n in range(6, 12)), 0.0)
    total = jnp.zeros((40, 128), jnp.float32)
    ends = jnp.zeros((8, 128), jnp.float32)
    for c in range(3):
        body = own[c] + near_z[c]
        body += jnp.where((lane >= 90) & (lane < 100), pltpu.roll(upper, 90 - 10 * c, 1), 0.0)
        body += jnp.where(lane < 10, pltpu.roll(lower, (128 - 10 * c) % 128, 1), 0.0)
        low, high = from_low[c : c + 1], from_high[c : c + 1]
        tile = jnp.where(sub == 0, low, jnp.where(sub == 1, high, 0.0))
        total += dot_right(jnp.concatenate([body, tile], axis=0), side[c])
        low = 0.75 * low + 0.25 * body[0:1]
        high = 0.75 * high + 0.25 * body[31:32]
        ends += jnp.where(sub == 2 + 2 * c, low, jnp.where(sub == 3 + 2 * c, high, 0.0))
    last = jnp.concatenate([total[24:32], jnp.where(sub < 2, total[32:40], ends)], axis=0)
    ghost_a[...] = total[0:24]
    ghost_a_in[0] = total[0:24]
    ghost_b[...] = last
    ghost_b_in[0] = last
    copies_a = gather(ghost_a, ghost_a_in, plane_peers, 2)
    copies_b = gather(ghost_b, ghost_b_in, line_peers, 3)
    indices[1].wait()

    def tiles(row, offset, source):
        def take(n, out):
            for s in range(SLOTS):
                at = tab[row, offset + n * SLOTS + s]
                out[s] = source[at >> 2, at & 3]

        return take

    def blocks(offset, source):
        def take(n, out):
            out[...] = source[tab[T_GHOST, offset + n * SLOTS]]

        return take

    arrive(planes_copies[0])
    planes_copies += (passed(tiles(T_PLANE, 0, planes_a_in), planes_a_to, planes_a_at, line_peers, 0),)
    arrive(planes_copies[1])
    planes_copies += (passed(tiles(T_PLANE, 32, planes_b_in), planes_b_to, planes_b_at, plane_peers, 1),)

    arrive(copies_a)
    ghost_copies = passed(blocks(0, ghost_a_in), ghost_a_to, ghost_a_at, line_peers, 2)
    arrive(copies_b)
    ghost_copies += passed(blocks(32, ghost_b_in), ghost_b_to, ghost_b_at, plane_peers, 3)
    arrive(planes_copies[2])
    arrive(planes_copies[3])
    arrive(ghost_copies)

    block = jnp.concatenate([ghost_a_at[tab[T_GHOST_AT, 0]], ghost_b_at[tab[T_GHOST_AT, 32]]], axis=0)
    pulled = dot_right(dot_left(along[...], block), spread[...])
    for q in range(SLOTS):
        pull[q] = pulled[q * F : q * F + F]
    faces = dot_right(block[32:40], face[...])

    lane = lax.broadcasted_iota(jnp.int32, (F, F * F), 1)
    row = lax.broadcasted_iota(jnp.int32, (F, F * F), 0)
    for s in range(SLOTS):
        rate = RATE * visc[s]
        ghosts = pull[tab[T_BOX, s]]
        active = tab[T_ACTIVE, s] > 0
        planes = (planes_a_at[tab[T_PLANE_AT, s], s], planes_b_at[tab[T_PLANE_AT, 32 + s], s])
        has_near = (tab[T_NEAR, s] > 0, tab[T_NEAR, 32 + s] > 0)
        for c in range(3):
            cells = fine[c, s]
            ends = [
                jnp.where(
                    has_near[d],
                    jnp.concatenate([planes[d][2 * c : 2 * c + 1], planes[d][2 * c + 1 : 2 * c + 2]], axis=1),
                    faces[2 + 2 * c + d : 3 + 2 * c + d],
                )
                for d in range(2)
            ]
            around = ghosts[:, c * F * F : (c + 1) * F * F] - 6.0 * cells
            around += jnp.where(row == 0, ends[0], pltpu.roll(cells, 1, 0))
            around += jnp.where(row == F - 1, ends[1], pltpu.roll(cells, F - 1, 0))
            around += jnp.where(lane < F, 0.0, pltpu.roll(cells, F, 1))
            around += jnp.where(lane >= F * F - F, 0.0, pltpu.roll(cells, F * F - F, 1))
            around += jnp.where(lane % F == 0, 0.0, pltpu.roll(cells, 1, 1))
            around += jnp.where(lane % F == F - 1, 0.0, pltpu.roll(cells, F * F - 1, 1))
            moved = cells + rate * around
            result[c, s] = jnp.where(active, moved, 0.0)
            adv[(c * SLOTS + s) * F : (c * SLOTS + s + 1) * F, :] = moved

    summed = dot_right(adv[...], pair_yz[...])
    mean = dot_left(pair_x[0], summed[:, 0:128]) + dot_left(pair_x[1], summed[:, 128:256])
    for s in range(SLOTS):
        for part, (out, out_in) in enumerate(((means_a, means_a_in), (means_b, means_b_in))):
            tile = mean[part * 32 + s * 8 : part * 32 + s * 8 + 6]
            out[s] = tile
            out_in[0, s] = tile
    facts = (spots[W_Y, 9], spots[W_Z, 9], tab[T_HERE, 0])
    facts = sum(jnp.where(lane[0:1] == n, v.astype(jnp.float32), 0.0) for n, v in enumerate(facts))
    result[2, SLOTS, 0:1, :] = facts
    copies_a = gather(means_a, means_a_in, plane_peers, 4)
    copies_b = gather(means_b, means_b_in, line_peers, 5)
    arrive(copies_a)
    means_copies = passed(tiles(T_MEAN, 0, means_a_in), means_a_to, means_a_at, line_peers, 4)
    arrive(copies_b)
    means_copies += passed(tiles(T_MEAN, 32, means_b_in), means_b_to, means_b_at, plane_peers, 5)
    arrive(means_copies)
    for q in range(SLOTS):
        spot = (SLOTS, slice(q // 2 * 8, q // 2 * 8 + 6), slice(q % 2 * 128, q % 2 * 128 + 128))
        result[0, *spot] = means_a_at[tab[T_MEAN_AT, q], q]
        result[1, *spot] = means_b_at[tab[T_MEAN_AT, 32 + q], q]
    for copy in started:
        copy.wait_send()


def place_kernel(result, coarse, fine_out, out, column, sems):
    fine_write = pltpu.make_async_copy(result.at[:, 0:SLOTS], fine_out, sems.at[8])
    fine_write.start()
    lane = lax.broadcasted_iota(jnp.int32, (8, 128), 1)
    facts = result[2, SLOTS, 0:1, 0:128]
    y, z, here = (jnp.sum(jnp.where(lane[0:1] == n, facts, 0.0)).astype(jnp.int32) for n in range(3))
    shift = z & 127
    keep = (lane >= shift) & (lane < shift + 8) & (here > 0)
    mine = (y >> 3) * 2 + (z >> 7)
    rest = []
    for n in range(8):
        part = (slice(None), slice(None), pl.ds(n // 2 * 8, 8), pl.ds(n % 2 * 128, 128))
        rest.append(pltpu.make_async_copy(coarse.at[part], out.at[part], sems.at[n]))
    for n in range(8):
        pl.when(mine != n)(rest[n].start)
    y = pl.multiple_of(y, 8)
    z = pl.multiple_of(z - shift, 128)
    writes = []
    for c in range(3):
        for q in range(SLOTS):
            for a in range(B):
                r = 2 * c + a // 2 % 2 + q // 2 * 8
                line = result[a // 4, SLOTS, r : r + 1, q % 2 * 128 : q % 2 * 128 + 128]
                line = jnp.broadcast_to(line, (8, 128))
                line = pltpu.roll(pltpu.roll(line, 72 - 64 * (a % 2), 1, stride=8, stride_axis=0), shift, 1)
                old = coarse[c, q * B + a, pl.ds(y, 8), pl.ds(z, 128)]
                column[c, q * B + a] = jnp.where(keep, line, old)
        spot = out.at[c, :, pl.ds(y, 8), pl.ds(z, 128)]
        writes.append(pltpu.make_async_copy(column.at[c], spot, sems.at[9 + c]))
        writes[-1].start()
    for n in range(8):
        pl.when(mine != n)(rest[n].wait)
    for copy in writes + [fine_write]:
        copy.wait()


def spec(space):
    return pl.BlockSpec(memory_space=space)


def on_device(coarse, fine, visc, corners, grid_slot, neighbors):
    f32 = jnp.float32
    dma = pltpu.SemaphoreType.DMA
    weights = [jnp.asarray(v, jnp.bfloat16) for v in constants()]
    tiles, a, b = (SLOTS, 6, 128), (24, 128), (16, 128)
    sides = (tiles, tiles, a, b, tiles, tiles)
    gathered = [((PLANE, LINE)[n % 2],) + shape for n, shape in enumerate(sides)]
    onward = [((LINE, PLANE)[n % 2],) + shape for n, shape in enumerate(sides)]
    result = pl.pallas_call(
        exchange_kernel,
        out_shape=jax.ShapeDtypeStruct((3, SLOTS + 1, F, F * F), f32),
        in_specs=[spec(pltpu.HBM)] * (6 + len(weights)),
        out_specs=spec(VMEM),
        scratch_shapes=[
            VMEM((3, corners.shape[0]), jnp.int32),
            VMEM((1, corners.shape[0]), jnp.int32),
            VMEM((2, corners.shape[0]), jnp.int32),
            VMEM(fine.shape, f32),
            VMEM(visc.shape, f32),
        ]
        + [VMEM(w.shape, w.dtype) for w in weights]
        + [
            VMEM((T_ROWS, 128), jnp.int32),
            pltpu.SMEM((T_ROWS, 128), jnp.int32),
            VMEM((W_ROWS, 128), jnp.int32),
            pltpu.SMEM((W_ROWS, 128), jnp.int32),
            VMEM((2, 3, 32, PITCH, 128), f32),
            VMEM((3, 32, 128), f32),
            VMEM((3, 32, 128), f32),
            VMEM((4, 32, 128), f32),
            VMEM((3, 32, 128), f32),
            VMEM((4, 32, 128), f32),
            VMEM((12, 8, 128), f32),
            VMEM((12, 8, 128), f32),
            VMEM((SLOTS, F, 3 * F * F), f32),
            VMEM((3 * SLOTS * F, F * F), f32),
        ]
        + [VMEM(shape, f32) for shape in (*sides, *gathered, *onward, *onward)]
        + [dma((5 + len(weights),)), dma((4,)), dma((5,)), dma((5,)), dma((12,)), dma((12,))]
        + [dma((6, PLANE))] * 4,
        compiler_params=pltpu.CompilerParams(collective_id=1, has_side_effects=True),
        name="exchange",
    )(
        corners.T, grid_slot.reshape(1, -1), neighbors.T, coarse, fine, visc,
        *weights,
    )
    return pl.pallas_call(
        place_kernel,
        out_shape=(jax.ShapeDtypeStruct(fine.shape, f32), jax.ShapeDtypeStruct(coarse.shape, f32)),
        in_specs=[spec(VMEM), spec(VMEM)],
        out_specs=(spec(pl.ANY), spec(pl.ANY)),
        scratch_shapes=[VMEM((3, 32, 8, 128), f32), dma((12,))],
        compiler_params=pltpu.CompilerParams(vmem_limit_bytes=16 << 20),
        name="place",
    )(result, coarse)


def solution(mesh):
    split = Mesh(
        mesh.devices.reshape(NXC, NZC, mesh.shape["gy"], mesh.shape["gz"]), ("gx_0", "gx_1", "gy", "gz")
    )
    in_specs = (
        P(None, GX, "gy", "gz"),
        P(None, GX_GY_GZ, None, None),
        P(GX_GY_GZ, None, None),
        P(),
        P(),
        P(),
    )
    out_specs = (P(None, GX_GY_GZ, None, None), P(None, GX, "gy", "gz"))
    return jax.shard_map(on_device, mesh=split, in_specs=in_specs, out_specs=out_specs, check_vma=False)
```
